32 devices in a mesh: copy: 4 (over z), row: 4 (over x, core), col: 2 (over y).
Axes of the slice: x: 2, y: 2, z: 4, core: 2. Of those that a mesh axis runs over, the one named last changes fastest.
Arguments:
- trailing: float32 [32768, 16, 2, 128], P(('copy', 'row'), None, 'col'), parts along dimension 0, may hold values from -6 to 6
- lower_trail: float32 [64, 2, 128, 768], P(('copy', 'row'), None, None, 'col'), parts along dimension 0, may hold values from -0.09375 to 0.09375
- lower_cross: float32 [384, 384], replicated, may hold values from -0.3125 to 0.3125
- panel_inverse: float32 [2, 384, 384], replicated, may hold values from -1 to 1, as said below
- target: float32 [32768, 2, 384], P(('copy', 'row'), None, 'col'), parts along dimension 0, may hold values from -6 to 6
Outputs:
- inverse_panels: float32 [32768, 2, 384], P(('copy', 'row'), None, 'col'), parts along dimension 0
The draws below stay inside these ranges and needn't reach their ends.
There are 4 independent parts, one for each index of `copy`. The reference program is written for one: setup_inputs(seed, part) draws one part's arguments, and reference() takes and returns one part's arrays. A program takes and returns all parts, laid end to end along the dimension named above; an argument that names none is the same for every part. Nothing has to cross between parts.
Inputs may be any that keep to these rules, and one draw needn't show every extreme that they name: `panel_inverse`: each of the two 384 x 384 matrices is unit lower triangular: ones on the diagonal, zeros above it.
All inputs are finite; a program needn't handle non-finite values.
Results may differ from the reference program's by a relative error of at most 0.000071.
Values sent between devices are 32-bit elements; how exact they have to be, the bound alone decides.
A program may use at most 192 MiB of HBM per device.

```python
import jax
import jax.numpy as jnp
from jax import lax

PW = 384
NB = 128
TQ = 16
ROWS = 8192
TRAIL = 4096
N_COL = 2


def draw_panel_inverse(key, part):
    strict_lower = jnp.tril(jnp.ones((PW, PW), jnp.float32), -1)
    values = jax.random.normal(key, (2, PW, PW), jnp.float32) / PW ** 0.5
    values = jnp.clip(values, -1.0, 1.0)
    return values * strict_lower + jnp.eye(PW, dtype=jnp.float32)


def block_scale(rng, shape, pieces, low, high):
    def one(dim, parts):
        draws = jax.random.uniform(jax.random.fold_in(jax.random.fold_in(rng, 6), dim), (parts,), jnp.float32, low / len(pieces), high / len(pieces))
        return jnp.repeat(jnp.exp(draws), shape[dim] // parts).reshape((-1,) + (1,) * (len(shape) - dim - 1))

    loudness = one(*pieces[0])
    for cut in pieces[1:]:
        loudness = loudness * one(*cut)
    return loudness


def normal_values(key, dims, deviation, reach, split=(), kind=jnp.bfloat16):
    array = deviation * jax.random.normal(key, dims, jnp.float32)
    if split:
        array = array * block_scale(key, dims, split, -0.22, 0.18)
    return jnp.clip(array, -reach, reach).astype(kind)


def setup_inputs(seed: int = 0, part: int = 0) -> dict:
    arg_keys = jax.random.split(jax.random.key(seed), 6)
    own_keys = jax.random.split(jax.random.fold_in(arg_keys[5], part), 6)
    return {
        "trailing": normal_values(own_keys[0], (ROWS, TQ, N_COL, NB), 1.0, 6.0, ((0, 4), (2, 2)), jnp.float32),
        "lower_trail": normal_values(own_keys[1], (TQ, N_COL, NB, 2 * PW), TRAIL ** -0.5, 0.09375, ((0, 4), (3, 2)), jnp.float32),
        "lower_cross": normal_values(arg_keys[2], (PW, PW), PW ** -0.5, 0.3125, (), jnp.float32),
        "panel_inverse": draw_panel_inverse(jax.random.fold_in(arg_keys[5], 71), part),
        "target": normal_values(own_keys[4], (ROWS, 2, PW), 1.0, 6.0, ((0, 4), (2, 2)), jnp.float32),
    }


precise = lax.Precision.HIGHEST


def matmul(first, second):
    return jnp.dot(first, second, preferred_element_type=jnp.float32, precision=precise)


def reference(trailing, lower_trail, lower_cross, panel_inverse, target):
    row_count = trailing.shape[0]
    trail_flat = trailing.reshape(row_count, trailing.shape[1] * trailing.shape[2] * trailing.shape[3])
    lower_flat = lower_trail.reshape(trail_flat.shape[1], lower_trail.shape[3])
    update = matmul(trail_flat, lower_flat)
    panel_cols = lower_flat.shape[1] // 2
    right_panel = matmul(target[:, 1, :] - update[:, panel_cols:], panel_inverse[1])
    left_panel = matmul(target[:, 0, :] - update[:, :panel_cols] - matmul(right_panel, lower_cross), panel_inverse[0])
    return jnp.stack([left_panel, right_panel], axis=1)
```

```python
import jax
import jax.numpy as jnp
from jax import lax
from jax.experimental import pallas as pl
from jax.experimental.pallas import tpu as pltpu
from jax.sharding import PartitionSpec as P

ROW_TILE = 256
LANES = 128
CHUNKS = 2
exact = lax.Precision.HIGHEST


def matmul(first, second, precision=lax.Precision.HIGH):
    return jnp.dot(first, second, preferred_element_type=jnp.float32, precision=precision)


def contract_last(first, second, precision=lax.Precision.HIGH):
    return lax.dot_general(
        first, second, (((1,), (1,)), ((), ())), preferred_element_type=jnp.float32, precision=precision
    )


def halves(value):
    high = value.astype(jnp.bfloat16)
    return high, (value - high.astype(jnp.float32)).astype(jnp.bfloat16)


def three_pass(first, second):
    first_high, first_low = first
    second_high, second_low = second

    def product(a, b):
        return jnp.dot(a, b, preferred_element_type=jnp.float32)

    return product(first_high, second_high) + (product(first_high, second_low) + product(first_low, second_high))


def share_kernel(trail_ref, factor_ref, weight_ref, target_ref, out_ref, high_ref, low_ref):
    @pl.when(pl.program_id(0) == 0)
    def _():
        high_ref[...], low_ref[...] = halves(factor_ref[...])

    blocks = trail_ref.shape[1]
    trail = jnp.concatenate([trail_ref[:, block, :] for block in range(blocks)], axis=1)
    summed = three_pass(halves(trail), (high_ref[...], low_ref[...]))
    start = three_pass(halves(weight_ref[...]), halves(target_ref[...]))
    out_ref[...] = start - summed.T


def share_of(trail, factor, weight, target, chunk=0, chunks=1):
    rows, blocks, width = trail.shape
    depth, out_cols = factor.shape
    in_cols = target.shape[0]
    count = rows // chunks
    tile = min(ROW_TILE, count)
    begin = chunk * (count // tile)
    return pl.pallas_call(
        share_kernel,
        grid=(count // tile,),
        in_specs=[
            pl.BlockSpec((tile, blocks, width), lambda i: (i + begin, 0, 0)),
            pl.BlockSpec((depth, out_cols), lambda i: (0, 0)),
            pl.BlockSpec((out_cols, in_cols), lambda i: (0, 0)),
            pl.BlockSpec((in_cols, tile), lambda i: (0, i + begin)),
        ],
        out_specs=pl.BlockSpec((out_cols, tile), lambda i: (0, i)),
        out_shape=jax.ShapeDtypeStruct((out_cols, count), jnp.float32),
        scratch_shapes=[pltpu.VMEM((depth, out_cols), jnp.bfloat16)] * 2,
        compiler_params=pltpu.CompilerParams(dimension_semantics=("arbitrary",)),
        cost_estimate=pl.CostEstimate(
            flops=6 * count * depth * out_cols, bytes_accessed=4 * count * depth, transcendentals=0
        ),
    )(trail, factor, weight, target)


MESH = pl.DeviceIdType.MESH
ROW_CHUNK = 256


def contract_bf16(first, second):
    return lax.dot_general(first, second, (((1,), (1,)), ((), ())), preferred_element_type=jnp.float32)


def three_pass_last(first, second):
    first_high, first_low = halves(first)
    second_high, second_low = halves(second)
    return contract_bf16(first_high, second_high) + (
        contract_bf16(first_high, second_low) + contract_bf16(first_low, second_high)
    )


def sweep_kernel(
    trail_ref, lower_ref, cross_ref, inverse_ref, target_ref, out_ref,
    stage, trail_high, trail_low, local, crossed, inverse, cross_in, target, turned, turned_own, fold,
    send_w, own_w, send_cat, own_cat, sums_out, sums_in, own,
    stage_sem, in_sem, target_sem, cross_send, cross_recv, gather_send, gather_recv, sum_send, sum_recv, out_sem,
):
    row = lax.axis_index("row")
    y = lax.axis_index("col")
    chip, core = row // 2, row % 2
    across = (1 - chip) * 2 + core
    twin = chip * 2 + (1 - core)
    across_twin = (1 - chip) * 2 + (1 - core)
    other = 1 - y
    pieces, height, panel = local.shape
    share = panel // 2
    rows, blocks, width = trail_ref.shape
    chunk = stage.shape[1]
    chunks = rows // chunk
    half = chunks // 2
    cut = share // LANES * LANES
    spans = (slice(cut, panel), slice(0, cut))

    barrier = pltpu.get_barrier_semaphore()
    for place in ({"col": other}, {"row": across}, {"row": twin}):
        pl.semaphore_signal(barrier, inc=1, device_id=place, device_id_type=MESH)

    def cross_copy(part, i):
        span = spans[part]
        return pltpu.make_async_remote_copy(
            src_ref=lower_ref.at[i, other, :, span],
            dst_ref=crossed.at[i, :, span],
            send_sem=cross_send.at[part, i],
            recv_sem=cross_recv.at[part, i],
            device_id={"col": other},
            device_id_type=MESH,
        )

    def stage_copy(c):
        return pltpu.make_async_copy(
            trail_ref.at[pl.ds(c * chunk, chunk)], stage.at[c % 2], stage_sem.at[c % 2]
        )

    def target_copy(c):
        return pltpu.make_async_copy(
            target_ref.at[:, pl.ds(pl.multiple_of(c * chunk, chunk), chunk)], target.at[c], target_sem.at[c]
        )

    inputs = (
        pltpu.make_async_copy(inverse_ref, inverse, in_sem.at[0]),
        pltpu.make_async_copy(cross_ref, cross_in, in_sem.at[1]),
        pltpu.make_async_copy(lower_ref.at[:, y], local, in_sem.at[2]),
    )
    for copy in inputs:
        copy.start()
    stage_copy(0).start()
    stage_copy(1).start()

    pl.semaphore_wait(barrier, 3)
    for part in range(2):
        for i in range(pieces):
            cross_copy(part, i).start()
    for c in range(chunks):
        target_copy(c).start()

    for copy in inputs:
        copy.wait()
    left, right = inverse[0], inverse[1]
    joint = -matmul(matmul(right, cross_in[...], exact), left, exact)
    cross_in[...] = joint
    for index, matrix in enumerate((left, right, joint)):
        turned[index] = matrix.T
    mine = pl.ds(pl.multiple_of(y * share, 8), share)
    for index in range(2):
        turned_own[index] = inverse[index, mine, :].T
    turned_own[2] = cross_in[mine, :].T

    is_left = y == 0
    for dest, owner in enumerate((other, y)):
        theirs = pl.ds(pl.multiple_of(owner * share, 8), share)
        to_left, to_right, joined = (turned[index, theirs, :] for index in range(3))
        nothing = jnp.zeros_like(to_right)
        fold[dest, 0, 0] = jnp.where(is_left, nothing, to_right)
        fold[dest, 0, 1] = jnp.where(is_left, to_right, nothing)
        fold[dest, 1, 0] = jnp.where(is_left, to_left, joined)
        fold[dest, 1, 1] = jnp.where(is_left, joined, to_left)

    def buffer(group):
        return own_w if group == 2 else send_w.at[group]

    def gather_copy(group, kind, i):
        source = across if kind == 2 else row
        spot = buffer(group).at[source * pieces + i]
        return pltpu.make_async_remote_copy(
            src_ref=spot,
            dst_ref=spot,
            send_sem=gather_send.at[group, kind, i],
            recv_sem=gather_recv.at[group, kind, i],
            device_id={"row": across if kind == 0 else twin},
            device_id_type=MESH,
        )

    def gather_arrived(group, kind, i):
        source = (across, twin, across_twin)[kind]
        spot = buffer(group).at[source * pieces + i]
        pltpu.make_async_remote_copy(
            src_ref=spot,
            dst_ref=spot,
            send_sem=gather_send.at[group, kind, i],
            recv_sem=gather_recv.at[group, kind, i],
            device_id={"row": across if kind == 0 else twin},
            device_id_type=MESH,
        ).wait_recv()

    def spread(group, i):
        gather_copy(group, 0, i).start()
        gather_copy(group, 1, i).start()

    def forward(group):
        def step(i, _):
            gather_arrived(group, 0, i)
            gather_copy(group, 2, i).start()
            return _

        lax.fori_loop(0, pieces, step, 0)

    def collect(group, held):
        def step(i, _):
            gather_arrived(group, 1, i)
            gather_arrived(group, 2, i)
            return _

        lax.fori_loop(0, pieces, step, 0)
        count = own_w.shape[1] if group == 2 else share
        for q in range(blocks):
            high, low = halves(buffer(group)[q])
            lanes = slice(q * width, (q + 1) * width)
            held[0:count, lanes] = high
            held[count : 2 * count, lanes] = low

    def convert(c):
        stage_copy(c).wait()
        here = pl.ds(pl.multiple_of(c * chunk, chunk), chunk)
        for block in range(blocks):
            high, low = halves(stage[c % 2, :, block, :])
            lanes = slice(block * width, (block + 1) * width)
            trail_high[here, lanes] = high
            trail_low[here, lanes] = low

        @pl.when(c + 2 < chunks)
        def _():
            stage_copy(c + 2).start()

    def summed(held, c):
        here = pl.ds(pl.multiple_of(c * chunk, chunk), chunk)
        count = held.shape[0] // 2
        both = contract_bf16(held[...], trail_high[here, :])
        return both[:count] + (both[count:] + contract_bf16(held[0:count, :], trail_low[here, :]))

    def begin(owner, group, c):
        theirs = pl.ds(pl.multiple_of(owner * share, 8), share)
        to_right = halves(target[c, share:panel, :])
        if group == 0:
            return three_pass(halves(turned_own[1, theirs, :]), to_right)
        to_left = halves(target[c, 0:share, :])
        return three_pass(halves(turned_own[0, theirs, :]), to_left) + three_pass(
            halves(turned_own[2, theirs, :]), to_right
        )

    def sum_copy(group, c):
        return pltpu.make_async_remote_copy(
            src_ref=sums_out.at[group, c],
            dst_ref=sums_in.at[group, c],
            send_sem=sum_send.at[group, c],
            recv_sem=sum_recv.at[group, c],
            device_id={"col": other},
            device_id_type=MESH,
        )

    def share_out(group, c):
        sums_out[group, c] = begin(other, group, c) - summed(send_cat.at[group], c)
        sum_copy(group, c).start()

    def fold_right(i, _):
        cross_copy(0, i).wait_recv()
        send_w[0, row * pieces + i] = three_pass_last(fold[0, 0, 0], local[i]) + three_pass_last(
            fold[0, 0, 1, :, spans[0]], crossed[i, :, spans[0]]
        )
        spread(0, i)
        convert(i)
        return _

    lax.fori_loop(0, pieces, fold_right, 0)
    forward(0)
    collect(0, send_cat.at[0])
    for c in range(chunks):
        target_copy(c).wait()

    def early(c, _):
        share_out(0, c)
        return _

    lax.fori_loop(0, half, early, 0)

    def fold_left(i, _):
        cross_copy(1, i).wait_recv()
        send_w[1, row * pieces + i] = three_pass_last(fold[0, 1, 0], local[i]) + three_pass_last(
            fold[0, 1, 1], crossed[i]
        )
        spread(1, i)
        convert(half + i)
        share_out(0, half + i)
        return _

    lax.fori_loop(0, pieces, fold_left, 0)

    def fold_own(i, _):
        for group in range(2):
            begins = (1 - group) * share
            own_w[row * pieces + i, begins : begins + share, :] = three_pass_last(
                fold[1, group, 0], local[i]
            ) + three_pass_last(fold[1, group, 1], crossed[i])
        spread(2, i)
        return _

    lax.fori_loop(0, pieces, fold_own, 0)
    forward(1)
    collect(1, send_cat.at[1])

    def late(c, _):
        share_out(1, c)
        return _

    lax.fori_loop(0, chunks, late, 0)
    forward(2)
    collect(2, own_cat)

    def mine_too(c, _):
        total = summed(own_cat, c)
        own[c, 0:share, :] = begin(y, 1, c) - total[0:share]
        own[c, share:panel, :] = begin(y, 0, c) - total[share:panel]
        return _

    lax.fori_loop(0, chunks, mine_too, 0)

    def out_copy(group, c):
        begins = (1 - group) * share
        return pltpu.make_async_copy(
            own.at[c, begins : begins + share, :],
            out_ref.at[begins : begins + share, pl.ds(pl.multiple_of(c * chunk, chunk), chunk)],
            out_sem.at[group, c],
        )

    for group in range(2):
        begins = (1 - group) * share

        def finish(c, _):
            sum_copy(group, c).wait_recv()
            own[c, begins : begins + share, :] += sums_in[group, c]
            out_copy(group, c).start()
            return _

        lax.fori_loop(0, chunks, finish, 0)

    def drain(i, _):
        for part in range(2):
            cross_copy(part, i).wait_send()
        for group in range(3):
            for kind in range(3):
                gather_copy(group, kind, i).wait_send()
        return _

    lax.fori_loop(0, pieces, drain, 0)

    def drain_sums(c, _):
        for group in range(2):
            sum_copy(group, c).wait_send()
            out_copy(group, c).wait()
        return _

    lax.fori_loop(0, chunks, drain_sums, 0)


def sweep(trailing, lower_trail, lower_cross, panel_inverse, target):
    rows, blocks, _, width = trailing.shape
    pieces, _, height, _ = lower_trail.shape
    panel = lower_cross.shape[0]
    share = panel // 2
    depth = blocks * width
    chunk = min(ROW_CHUNK, rows // 8)
    chunks = rows // chunk
    held = target.transpose(1, 2, 0).reshape(panel, rows)
    f32, bf16 = jnp.float32, jnp.bfloat16
    vmem, dma = pltpu.VMEM, pltpu.SemaphoreType.DMA
    out = pl.pallas_call(
        sweep_kernel,
        in_specs=[pl.BlockSpec(memory_space=pl.ANY)] * 5,
        out_specs=pl.BlockSpec(memory_space=pl.ANY),
        out_shape=jax.ShapeDtypeStruct((panel, rows), f32),
        scratch_shapes=[
            vmem((2, chunk, blocks, width), f32),
            vmem((rows, depth), bf16),
            vmem((rows, depth), bf16),
            vmem((pieces, height, panel), f32),
            vmem((pieces, height, panel), f32),
            vmem((2, panel, panel), f32),
            vmem((panel, panel), f32),
            vmem((chunks, panel, chunk), f32),
            vmem((3, panel, panel), f32),
            vmem((3, panel, share), f32),
            vmem((2, 2, 2, share, panel), f32),
            vmem((2, blocks, share, width), f32),
            vmem((blocks, panel, width), f32),
            vmem((2, panel, depth), bf16),
            vmem((2 * panel, depth), bf16),
            vmem((2, chunks, share, chunk), f32),
            vmem((2, chunks, share, chunk), f32),
            vmem((chunks, panel, chunk), f32),
            dma((2,)),
            dma((3,)),
            dma((chunks,)),
            dma((2, pieces)),
            dma((2, pieces)),
            dma((3, 3, pieces)),
            dma((3, 3, pieces)),
            dma((2, chunks)),
            dma((2, chunks)),
            dma((2, chunks)),
        ],
        compiler_params=pltpu.CompilerParams(
            collective_id=0, has_side_effects=True, vmem_limit_bytes=62 * 1024 * 1024
        ),
    )(trailing.reshape(rows, blocks, width), lower_trail, lower_cross, panel_inverse, held)
    return out.reshape(2, share, rows).transpose(2, 0, 1)


def fits(trailing, lower_trail, lower_cross):
    rows, blocks, _, width = trailing.shape
    pieces, owners, height, held = lower_trail.shape
    panel = lower_cross.shape[0]
    return (
        lax.axis_size("row") == 4
        and lax.axis_size("col") == 2
        and owners == 2
        and held == panel
        and height == width == LANES
        and blocks == 4 * pieces
        and panel % LANES == 0
        and panel % 32 == 0
        and rows % (8 * LANES) == 0
        and rows // min(ROW_CHUNK, rows // 8) == 2 * pieces
    )


def per_device(trailing, lower_trail, lower_cross, panel_inverse, target):
    if fits(trailing, lower_trail, lower_cross):
        return sweep(trailing, lower_trail, lower_cross, panel_inverse, target)
    cols = lax.axis_size("col")
    me = lax.axis_index("col")
    rows, blocks, _, width = trailing.shape
    depth = lower_trail.shape[0] * width
    panel = lower_cross.shape[0]
    span = 2 * panel
    share = panel // cols
    out_cols = 2 * share
    held = span // cols

    def shift(array, step):
        if step == 0:
            return array
        return lax.ppermute(array, "col", [(i, (i + step) % cols) for i in range(cols)])

    pieces = []
    for step in range(cols):
        block = lax.dynamic_index_in_dim(lower_trail, (me + step) % cols, 1, keepdims=False)
        pieces.append(shift(block, step).reshape(depth, held))

    left, right = panel_inverse[0], panel_inverse[1]
    cross = matmul(matmul(right, lower_cross, exact), left, exact)
    top = jnp.concatenate([left.T, -cross.T], axis=1)
    bottom = jnp.concatenate([jnp.zeros_like(left), right.T], axis=1)
    by_owner = jnp.stack([top, bottom]).reshape(2, cols, share, span)

    def owner_fold(owner):
        return lax.dynamic_index_in_dim(by_owner, owner, 1, keepdims=False).reshape(out_cols, span)

    def gathered(fold, part):
        total = None
        for back, piece in enumerate(pieces):
            source = (me - back) % cols
            weights = lax.dynamic_slice_in_dim(fold[part], source * held, held, 1)
            term = contract_last(piece, weights)
            total = term if total is None else total + term
        return lax.all_gather(total, "row", axis=0, tiled=True)

    held_col = jnp.arange(out_cols)
    place = (held_col // share) * panel + me * share + held_col % share
    pick = (place[:, None] == jnp.arange(span)[None, :]).astype(jnp.float32)

    trail = trailing.reshape(rows, blocks, width)
    own_target = target.transpose(1, 2, 0).reshape(out_cols, rows)
    first = LANES if out_cols > LANES else out_cols
    parts = [slice(0, first)] + ([slice(first, out_cols)] if first < out_cols else [])
    folds = [owner_fold((me + step) % cols) for step in range(cols)]
    factors = {}
    for step in range(1, cols):
        for index, part in enumerate(parts):
            factors[step, index] = gathered(folds[step], part)
    own_factor = gathered(folds[0], slice(0, out_cols))

    chunks = CHUNKS if rows % (CHUNKS * LANES) == 0 else 1
    arrived = [[[] for _ in range(chunks)] for _ in parts]
    for step in range(1, cols):
        weights = contract_last(folds[step], pick, exact)
        for index, part in enumerate(parts):
            for chunk in range(chunks):
                partial = share_of(trail, factors[step, index], weights[part], own_target, chunk, chunks)
                arrived[index][chunk].append(shift(partial, step))
    own = share_of(trail, own_factor, contract_last(folds[0], pick, exact), own_target)
    if cols == 1:
        return own.reshape(2, share, rows).transpose(2, 0, 1)
    others = []
    for pieces_here in arrived:
        sums = [sum(group[1:], group[0]) for group in pieces_here]
        others.append(jnp.concatenate(sums, axis=1))
    result = own + jnp.concatenate(others, axis=0)
    return result.reshape(2, share, rows).transpose(2, 0, 1)


def solution(mesh):
    placed = (
        P(("copy", "row"), None, "col", None),
        P(("copy", "row"), None, None, "col"),
        P(),
        P(),
        P(("copy", "row"), None, "col"),
    )
    return jax.shard_map(
        per_device,
        mesh=mesh,
        in_specs=placed,
        out_specs=P(("copy", "row"), None, "col"),
        check_vma=False,
    )
```

```python
import jax
import jax.numpy as jnp
from jax import lax
from jax.experimental import pallas as pl
from jax.experimental.pallas import tpu as pltpu
from jax.sharding import PartitionSpec as P

ROW_TILE = 256
LANES = 128
CHUNKS = 2
exact = lax.Precision.HIGHEST


def matmul(first, second, precision=lax.Precision.HIGH):
    return jnp.dot(first, second, preferred_element_type=jnp.float32, precision=precision)


def contract_last(first, second, precision=lax.Precision.HIGH):
    return lax.dot_general(
        first, second, (((1,), (1,)), ((), ())), preferred_element_type=jnp.float32, precision=precision
    )


def halves(value):
    high = value.astype(jnp.bfloat16)
    return high, (value - high.astype(jnp.float32)).astype(jnp.bfloat16)


def three_pass(first, second):
    first_high, first_low = first
    second_high, second_low = second

    def product(a, b):
        return jnp.dot(a, b, preferred_element_type=jnp.float32)

    return product(first_high, second_high) + (product(first_high, second_low) + product(first_low, second_high))


def share_kernel(trail_ref, factor_ref, weight_ref, target_ref, out_ref, high_ref, low_ref):
    @pl.when(pl.program_id(0) == 0)
    def _():
        high_ref[...], low_ref[...] = halves(factor_ref[...])

    blocks = trail_ref.shape[1]
    trail = jnp.concatenate([trail_ref[:, block, :] for block in range(blocks)], axis=1)
    summed = three_pass(halves(trail), (high_ref[...], low_ref[...]))
    start = three_pass(halves(weight_ref[...]), halves(target_ref[...]))
    out_ref[...] = start - summed.T


def share_of(trail, factor, weight, target, chunk=0, chunks=1):
    rows, blocks, width = trail.shape
    depth, out_cols = factor.shape
    in_cols = target.shape[0]
    count = rows // chunks
    tile = min(ROW_TILE, count)
    begin = chunk * (count // tile)
    return pl.pallas_call(
        share_kernel,
        grid=(count // tile,),
        in_specs=[
            pl.BlockSpec((tile, blocks, width), lambda i: (i + begin, 0, 0)),
            pl.BlockSpec((depth, out_cols), lambda i: (0, 0)),
            pl.BlockSpec((out_cols, in_cols), lambda i: (0, 0)),
            pl.BlockSpec((in_cols, tile), lambda i: (0, i + begin)),
        ],
        out_specs=pl.BlockSpec((out_cols, tile), lambda i: (0, i)),
        out_shape=jax.ShapeDtypeStruct((out_cols, count), jnp.float32),
        scratch_shapes=[pltpu.VMEM((depth, out_cols), jnp.bfloat16)] * 2,
        compiler_params=pltpu.CompilerParams(dimension_semantics=("arbitrary",)),
        cost_estimate=pl.CostEstimate(
            flops=6 * count * depth * out_cols, bytes_accessed=4 * count * depth, transcendentals=0
        ),
    )(trail, factor, weight, target)


MESH = pl.DeviceIdType.MESH
ROW_CHUNK = 256


def contract_bf16(first, second):
    return lax.dot_general(first, second, (((1,), (1,)), ((), ())), preferred_element_type=jnp.float32)


def three_pass_last(first, second):
    first_high, first_low = halves(first)
    second_high, second_low = halves(second)
    return contract_bf16(first_high, second_high) + (
        contract_bf16(first_high, second_low) + contract_bf16(first_low, second_high)
    )


def sweep_kernel(
    trail_ref, lower_ref, cross_ref, inverse_ref, target_ref, out_ref,
    stage, trail_high, trail_low, local, crossed, inverse, cross_in, target, turned, turned_own, fold,
    send_w, own_w, send_cat, own_cat, sums_out, sums_in,
    stage_sem, in_sem, target_sem, cross_send, cross_recv, gather_send, gather_recv, sum_send, sum_recv,
):
    row = lax.axis_index("row")
    y = lax.axis_index("col")
    chip, core = row // 2, row % 2
    across = (1 - chip) * 2 + core
    twin = chip * 2 + (1 - core)
    across_twin = (1 - chip) * 2 + (1 - core)
    other = 1 - y
    pieces, height, panel = local.shape
    share = panel // 2
    rows, blocks, width = trail_ref.shape
    chunk = stage.shape[2]
    chunks = rows // chunk
    cut = share // LANES * LANES
    spans = (slice(cut, panel), slice(0, cut))

    barrier = pltpu.get_barrier_semaphore()
    for place in ({"col": other}, {"row": across}, {"row": twin}):
        pl.semaphore_signal(barrier, inc=1, device_id=place, device_id_type=MESH)

    def cross_copy(part, i):
        span = spans[part]
        return pltpu.make_async_remote_copy(
            src_ref=lower_ref.at[i, other, :, span],
            dst_ref=crossed.at[i, :, span],
            send_sem=cross_send.at[part, i],
            recv_sem=cross_recv.at[part, i],
            device_id={"col": other},
            device_id_type=MESH,
        )

    def stage_copy(c, block):
        return pltpu.make_async_copy(
            trail_ref.at[pl.ds(c * chunk, chunk), block], stage.at[c % 2, block], stage_sem.at[c % 2, block]
        )

    def stage_chunk(c):
        for block in range(blocks):
            stage_copy(c, block).start()

    def target_copy(c):
        return pltpu.make_async_copy(
            target_ref.at[:, pl.ds(pl.multiple_of(c * chunk, chunk), chunk)], target.at[c], target_sem.at[c]
        )

    inputs = (
        pltpu.make_async_copy(inverse_ref, inverse, in_sem.at[0]),
        pltpu.make_async_copy(cross_ref, cross_in, in_sem.at[1]),
        pltpu.make_async_copy(lower_ref.at[:, y], local, in_sem.at[2]),
    )
    for copy in inputs:
        copy.start()
    pl.semaphore_wait(barrier, 3)
    for part in range(2):
        for i in range(pieces):
            cross_copy(part, i).start()
    stage_chunk(0)
    stage_chunk(1)
    for c in range(chunks):
        target_copy(c).start()

    for copy in inputs:
        copy.wait()
    left, right = inverse[0], inverse[1]
    joint = -matmul(matmul(right, cross_in[...], exact), left, exact)
    cross_in[...] = joint
    for index, matrix in enumerate((left, right, joint)):
        turned[index] = matrix.T
    mine = pl.ds(pl.multiple_of(y * share, 8), share)
    for index in range(2):
        turned_own[index] = inverse[index, mine, :].T
    turned_own[2] = cross_in[mine, :].T

    is_left = y == 0
    for dest, owner in enumerate((other, y)):
        theirs = pl.ds(pl.multiple_of(owner * share, 8), share)
        to_left, to_right, joined = (turned[index, theirs, :] for index in range(3))
        nothing = jnp.zeros_like(to_right)
        fold[dest, 0, 0] = jnp.where(is_left, nothing, to_right)
        fold[dest, 0, 1] = jnp.where(is_left, to_right, nothing)
        fold[dest, 1, 0] = jnp.where(is_left, to_left, joined)
        fold[dest, 1, 1] = jnp.where(is_left, joined, to_left)

    def buffer(group):
        return own_w if group == 2 else send_w.at[group]

    def gather_copy(group, kind, i):
        source = across if kind == 2 else row
        spot = buffer(group).at[source * pieces + i]
        return pltpu.make_async_remote_copy(
            src_ref=spot,
            dst_ref=spot,
            send_sem=gather_send.at[group, kind, i],
            recv_sem=gather_recv.at[group, kind, i],
            device_id={"row": across if kind == 0 else twin},
            device_id_type=MESH,
        )

    def gather_arrived(group, kind, i):
        source = (across, twin, across_twin)[kind]
        spot = buffer(group).at[source * pieces + i]
        pltpu.make_async_remote_copy(
            src_ref=spot,
            dst_ref=spot,
            send_sem=gather_send.at[group, kind, i],
            recv_sem=gather_recv.at[group, kind, i],
            device_id={"row": across if kind == 0 else twin},
            device_id_type=MESH,
        ).wait_recv()

    def spread(group, i):
        gather_copy(group, 0, i).start()
        gather_copy(group, 1, i).start()

    def forward(group):
        def step(i, _):
            gather_arrived(group, 0, i)
            gather_copy(group, 2, i).start()
            return _

        lax.fori_loop(0, pieces, step, 0)

    def collect(group, held):
        def step(i, _):
            gather_arrived(group, 1, i)
            gather_arrived(group, 2, i)
            return _

        lax.fori_loop(0, pieces, step, 0)
        count = own_w.shape[1] if group == 2 else share
        for q in range(blocks):
            high, low = halves(buffer(group)[q])
            lanes = slice(q * width, (q + 1) * width)
            held[0:count, lanes] = high
            held[count : 2 * count, lanes] = low

    def convert(c):
        for block in range(blocks):
            stage_copy(c, block).wait()
        here = pl.ds(pl.multiple_of(c * chunk, chunk), chunk)
        for block in range(blocks):
            high, low = halves(stage[c % 2, block])
            lanes = slice(block * width, (block + 1) * width)
            trail_high[here, lanes] = high
            trail_low[here, lanes] = low

        @pl.when(c + 2 < chunks)
        def _():
            stage_chunk(c + 2)

    def summed(held, c):
        here = pl.ds(pl.multiple_of(c * chunk, chunk), chunk)
        count = held.shape[0] // 2
        both = contract_bf16(held[...], trail_high[here, :])
        return both[:count] + (both[count:] + contract_bf16(held[0:count, :], trail_low[here, :]))

    def begin(owner, group, c):
        theirs = pl.ds(pl.multiple_of(owner * share, 8), share)
        to_right = halves(target[c, share:panel, :])
        if group == 0:
            return three_pass(halves(turned_own[1, theirs, :]), to_right)
        to_left = halves(target[c, 0:share, :])
        return three_pass(halves(turned_own[0, theirs, :]), to_left) + three_pass(
            halves(turned_own[2, theirs, :]), to_right
        )

    def sum_copy(group, c):
        return pltpu.make_async_remote_copy(
            src_ref=sums_out.at[group, c],
            dst_ref=sums_in.at[group, c],
            send_sem=sum_send.at[group, c],
            recv_sem=sum_recv.at[group, c],
            device_id={"col": other},
            device_id_type=MESH,
        )

    def share_out(group, c):
        sums_out[group, c] = begin(other, group, c) - summed(send_cat.at[group], c)
        sum_copy(group, c).start()

    def fold_right(i, _):
        cross_copy(0, i).wait_recv()
        send_w[0, row * pieces + i] = three_pass_last(fold[0, 0, 0], local[i]) + three_pass_last(
            fold[0, 0, 1, :, spans[0]], crossed[i, :, spans[0]]
        )
        spread(0, i)
        convert(2 * i)
        convert(2 * i + 1)
        return _

    lax.fori_loop(0, pieces, fold_right, 0)
    forward(0)
    collect(0, send_cat.at[0])
    for c in range(chunks):
        target_copy(c).wait()

    def early(c, _):
        share_out(0, c)
        return _

    lax.fori_loop(0, chunks, early, 0)

    def fold_left(i, _):
        cross_copy(1, i).wait_recv()
        send_w[1, row * pieces + i] = three_pass_last(fold[0, 1, 0], local[i]) + three_pass_last(
            fold[0, 1, 1], crossed[i]
        )
        spread(1, i)
        return _

    lax.fori_loop(0, pieces, fold_left, 0)

    def fold_own(i, _):
        for group in range(2):
            begins = (1 - group) * share
            own_w[row * pieces + i, begins : begins + share, :] = three_pass_last(
                fold[1, group, 0], local[i]
            ) + three_pass_last(fold[1, group, 1], crossed[i])
        spread(2, i)
        return _

    lax.fori_loop(0, pieces, fold_own, 0)
    forward(1)
    collect(1, send_cat.at[1])

    def late(c, _):
        share_out(1, c)
        return _

    lax.fori_loop(0, chunks, late, 0)
    forward(2)
    collect(2, own_cat)

    def mine_too(c, _):
        total = summed(own_cat, c)
        here = pl.ds(pl.multiple_of(c * chunk, chunk), chunk)
        out_ref[0:share, here] = begin(y, 1, c) - total[0:share]
        out_ref[share:panel, here] = begin(y, 0, c) - total[share:panel]
        return _

    lax.fori_loop(0, chunks, mine_too, 0)

    for group in range(2):
        begins = (1 - group) * share

        def finish(c, _):
            sum_copy(group, c).wait_recv()
            here = pl.ds(pl.multiple_of(c * chunk, chunk), chunk)
            out_ref[begins : begins + share, here] += sums_in[group, c]
            return _

        lax.fori_loop(0, chunks, finish, 0)

    def drain(i, _):
        for part in range(2):
            cross_copy(part, i).wait_send()
        for group in range(3):
            for kind in range(3):
                gather_copy(group, kind, i).wait_send()
        return _

    lax.fori_loop(0, pieces, drain, 0)

    def drain_sums(c, _):
        for group in range(2):
            sum_copy(group, c).wait_send()
        return _

    lax.fori_loop(0, chunks, drain_sums, 0)


def sweep(trailing, lower_trail, lower_cross, panel_inverse, target):
    rows, blocks, _, width = trailing.shape
    pieces, _, height, _ = lower_trail.shape
    panel = lower_cross.shape[0]
    share = panel // 2
    depth = blocks * width
    chunk = min(ROW_CHUNK, rows // 8)
    chunks = rows // chunk
    held = target.transpose(1, 2, 0).reshape(panel, rows)
    f32, bf16 = jnp.float32, jnp.bfloat16
    vmem, dma = pltpu.VMEM, pltpu.SemaphoreType.DMA
    out = pl.pallas_call(
        sweep_kernel,
        in_specs=[pl.BlockSpec(memory_space=pl.ANY)] * 5,
        out_specs=pl.BlockSpec(memory_space=pltpu.VMEM),
        out_shape=vmem((panel, rows), f32),
        scratch_shapes=[
            vmem((2, blocks, chunk, width), f32),
            vmem((rows, depth), bf16),
            vmem((rows, depth), bf16),
            vmem((pieces, height, panel), f32),
            vmem((pieces, height, panel), f32),
            vmem((2, panel, panel), f32),
            vmem((panel, panel), f32),
            vmem((chunks, panel, chunk), f32),
            vmem((3, panel, panel), f32),
            vmem((3, panel, share), f32),
            vmem((2, 2, 2, share, panel), f32),
            vmem((2, blocks, share, width), f32),
            vmem((blocks, panel, width), f32),
            vmem((2, panel, depth), bf16),
            vmem((2 * panel, depth), bf16),
            vmem((2, chunks, share, chunk), f32),
            vmem((2, chunks, share, chunk), f32),
            dma((2, blocks)),
            dma((3,)),
            dma((chunks,)),
            dma((2, pieces)),
            dma((2, pieces)),
            dma((3, 3, pieces)),
            dma((3, 3, pieces)),
            dma((2, chunks)),
            dma((2, chunks)),
        ],
        compiler_params=pltpu.CompilerParams(
            collective_id=0, has_side_effects=True, vmem_limit_bytes=56 * 1024 * 1024
        ),
    )(trailing.reshape(rows, blocks, width), lower_trail, lower_cross, panel_inverse, held)
    return out.reshape(2, share, rows).transpose(2, 0, 1)


def fits(trailing, lower_trail, lower_cross):
    rows, blocks, _, width = trailing.shape
    pieces, owners, height, held = lower_trail.shape
    panel = lower_cross.shape[0]
    return (
        lax.axis_size("row") == 4
        and lax.axis_size("col") == 2
        and owners == 2
        and held == panel
        and height == width == LANES
        and blocks == 4 * pieces
        and panel % LANES == 0
        and panel % 32 == 0
        and rows % (8 * LANES) == 0
        and rows // min(ROW_CHUNK, rows // 8) == 2 * pieces
    )


def per_device(trailing, lower_trail, lower_cross, panel_inverse, target):
    if fits(trailing, lower_trail, lower_cross):
        return sweep(trailing, lower_trail, lower_cross, panel_inverse, target)
    cols = lax.axis_size("col")
    me = lax.axis_index("col")
    rows, blocks, _, width = trailing.shape
    depth = lower_trail.shape[0] * width
    panel = lower_cross.shape[0]
    span = 2 * panel
    share = panel // cols
    out_cols = 2 * share
    held = span // cols

    def shift(array, step):
        if step == 0:
            return array
        return lax.ppermute(array, "col", [(i, (i + step) % cols) for i in range(cols)])

    pieces = []
    for step in range(cols):
        block = lax.dynamic_index_in_dim(lower_trail, (me + step) % cols, 1, keepdims=False)
        pieces.append(shift(block, step).reshape(depth, held))

    left, right = panel_inverse[0], panel_inverse[1]
    cross = matmul(matmul(right, lower_cross, exact), left, exact)
    top = jnp.concatenate([left.T, -cross.T], axis=1)
    bottom = jnp.concatenate([jnp.zeros_like(left), right.T], axis=1)
    by_owner = jnp.stack([top, bottom]).reshape(2, cols, share, span)

    def owner_fold(owner):
        return lax.dynamic_index_in_dim(by_owner, owner, 1, keepdims=False).reshape(out_cols, span)

    def gathered(fold, part):
        total = None
        for back, piece in enumerate(pieces):
            source = (me - back) % cols
            weights = lax.dynamic_slice_in_dim(fold[part], source * held, held, 1)
            term = contract_last(piece, weights)
            total = term if total is None else total + term
        return lax.all_gather(total, "row", axis=0, tiled=True)

    held_col = jnp.arange(out_cols)
    place = (held_col // share) * panel + me * share + held_col % share
    pick = (place[:, None] == jnp.arange(span)[None, :]).astype(jnp.float32)

    trail = trailing.reshape(rows, blocks, width)
    own_target = target.transpose(1, 2, 0).reshape(out_cols, rows)
    first = LANES if out_cols > LANES else out_cols
    parts = [slice(0, first)] + ([slice(first, out_cols)] if first < out_cols else [])
    folds = [owner_fold((me + step) % cols) for step in range(cols)]
    factors = {}
    for step in range(1, cols):
        for index, part in enumerate(parts):
            factors[step, index] = gathered(folds[step], part)
    own_factor = gathered(folds[0], slice(0, out_cols))

    chunks = CHUNKS if rows % (CHUNKS * LANES) == 0 else 1
    arrived = [[[] for _ in range(chunks)] for _ in parts]
    for step in range(1, cols):
        weights = contract_last(folds[step], pick, exact)
        for index, part in enumerate(parts):
            for chunk in range(chunks):
                partial = share_of(trail, factors[step, index], weights[part], own_target, chunk, chunks)
                arrived[index][chunk].append(shift(partial, step))
    own = share_of(trail, own_factor, contract_last(folds[0], pick, exact), own_target)
    if cols == 1:
        return own.reshape(2, share, rows).transpose(2, 0, 1)
    others = []
    for pieces_here in arrived:
        sums = [sum(group[1:], group[0]) for group in pieces_here]
        others.append(jnp.concatenate(sums, axis=1))
    result = own + jnp.concatenate(others, axis=0)
    return result.reshape(2, share, rows).transpose(2, 0, 1)


def solution(mesh):
    placed = (
        P(("copy", "row"), None, "col", None),
        P(("copy", "row"), None, None, "col"),
        P(),
        P(),
        P(("copy", "row"), None, "col"),
    )
    return jax.shard_map(
        per_device,
        mesh=mesh,
        in_specs=placed,
        out_specs=P(("copy", "row"), None, "col"),
        check_vma=False,
    )
```

```python
import jax
import jax.numpy as jnp
from jax import lax
from jax.experimental import pallas as pl
from jax.experimental.pallas import tpu as pltpu
from jax.sharding import PartitionSpec as P

ROW_TILE = 256
LANES = 128
CHUNKS = 2
exact = lax.Precision.HIGHEST


def matmul(first, second, precision=lax.Precision.HIGH):
    return jnp.dot(first, second, preferred_element_type=jnp.float32, precision=precision)


def contract_last(first, second, precision=lax.Precision.HIGH):
    return lax.dot_general(
        first, second, (((1,), (1,)), ((), ())), preferred_element_type=jnp.float32, precision=precision
    )


def halves(value):
    high = value.astype(jnp.bfloat16)
    return high, (value - high.astype(jnp.float32)).astype(jnp.bfloat16)


def three_pass(first, second):
    first_high, first_low = first
    second_high, second_low = second

    def product(a, b):
        return jnp.dot(a, b, preferred_element_type=jnp.float32)

    return product(first_high, second_high) + (product(first_high, second_low) + product(first_low, second_high))


def share_kernel(trail_ref, factor_ref, weight_ref, target_ref, out_ref, high_ref, low_ref):
    @pl.when(pl.program_id(0) == 0)
    def _():
        high_ref[...], low_ref[...] = halves(factor_ref[...])

    blocks = trail_ref.shape[1]
    trail = jnp.concatenate([trail_ref[:, block, :] for block in range(blocks)], axis=1)
    summed = three_pass(halves(trail), (high_ref[...], low_ref[...]))
    start = three_pass(halves(weight_ref[...]), halves(target_ref[...]))
    out_ref[...] = start - summed.T


def share_of(trail, factor, weight, target, chunk=0, chunks=1):
    rows, blocks, width = trail.shape
    depth, out_cols = factor.shape
    in_cols = target.shape[0]
    count = rows // chunks
    tile = min(ROW_TILE, count)
    begin = chunk * (count // tile)
    return pl.pallas_call(
        share_kernel,
        grid=(count // tile,),
        in_specs=[
            pl.BlockSpec((tile, blocks, width), lambda i: (i + begin, 0, 0)),
            pl.BlockSpec((depth, out_cols), lambda i: (0, 0)),
            pl.BlockSpec((out_cols, in_cols), lambda i: (0, 0)),
            pl.BlockSpec((in_cols, tile), lambda i: (0, i + begin)),
        ],
        out_specs=pl.BlockSpec((out_cols, tile), lambda i: (0, i)),
        out_shape=jax.ShapeDtypeStruct((out_cols, count), jnp.float32),
        scratch_shapes=[pltpu.VMEM((depth, out_cols), jnp.bfloat16)] * 2,
        compiler_params=pltpu.CompilerParams(dimension_semantics=("arbitrary",)),
        cost_estimate=pl.CostEstimate(
            flops=6 * count * depth * out_cols, bytes_accessed=4 * count * depth, transcendentals=0
        ),
    )(trail, factor, weight, target)


MESH = pl.DeviceIdType.MESH
ROW_CHUNK = 256


def contract_bf16(first, second):
    return lax.dot_general(first, second, (((1,), (1,)), ((), ())), preferred_element_type=jnp.float32)


def three_pass_last(first, second):
    first_high, first_low = halves(first)
    second_high, second_low = halves(second)
    return contract_bf16(first_high, second_high) + (
        contract_bf16(first_high, second_low) + contract_bf16(first_low, second_high)
    )


def sweep_kernel(
    trail_ref, lower_ref, cross_ref, inverse_ref, target_ref, out_ref,
    stage, trail_high, trail_low, local, leaving, packed, parcel, crossed, inverse, cross_in, target, turned, turned_own, fold,
    send_w, own_w, send_cat, own_cat, sums_out, sums_in,
    stage_sem, in_sem, target_sem, cross_send, cross_recv, gather_send, far_recv, near_recv, sum_send, sum_recv,
):
    row = lax.axis_index("row")
    y = lax.axis_index("col")
    chip, core = row // 2, row % 2
    across = (1 - chip) * 2 + core
    twin = chip * 2 + (1 - core)
    across_twin = (1 - chip) * 2 + (1 - core)
    other = 1 - y
    pieces, height, panel = local.shape
    share = panel // 2
    rows, blocks, width = trail_ref.shape
    chunk = stage.shape[2]
    chunks = rows // chunk
    cut = share // LANES * LANES
    rest = cut + LANES
    odd = share - cut
    low_rows, high_rows = slice(0, height // 2), slice(height // 2, height)
    is_low = lax.broadcasted_iota(jnp.int32, (height // 2, LANES), 1) < odd

    barrier = pltpu.get_barrier_semaphore()
    for place in ({"col": other}, {"row": across}, {"row": twin}):
        pl.semaphore_signal(barrier, inc=1, device_id=place, device_id_type=MESH)

    def settle(ref, sem):
        pltpu.make_async_copy(ref, ref, sem).wait()

    def turn(value):
        return pltpu.roll(value, odd, 1)

    def cross_copy(part, i):
        return pltpu.make_async_remote_copy(
            src_ref=packed.at[part, i],
            dst_ref=parcel.at[part, i],
            send_sem=cross_send.at[0],
            recv_sem=cross_recv.at[i if part == 0 else pieces],
            device_id={"col": other},
            device_id_type=MESH,
        )

    def cross_out(part):
        def step(i, carry):
            upper = leaving[i, low_rows, cut:rest]
            lower = leaving[i, high_rows, cut:rest]
            if part == 0:
                packed[0, i, 0:height, :] = leaving[i, :, rest:panel]
                packed[0, i, height:share, :] = jnp.where(is_low, turn(upper), lower)
            else:
                packed[1, i, 0:height, :] = leaving[i, :, 0:cut]
                packed[1, i, height:share, :] = jnp.where(is_low, upper, turn(lower))
            cross_copy(part, i).start()
            return carry

        lax.fori_loop(0, pieces, step, 0)

    def stage_copy(c, block):
        return pltpu.make_async_copy(
            trail_ref.at[pl.ds(c * chunk, chunk), block], stage.at[c % 2, block], stage_sem.at[c % 2]
        )

    def stage_chunk(c):
        for block in range(blocks):
            stage_copy(c, block).start()

    def target_copy(c):
        return pltpu.make_async_copy(
            target_ref.at[:, pl.ds(pl.multiple_of(c * chunk, chunk), chunk)], target.at[c], target_sem.at[0]
        )

    inputs = (
        pltpu.make_async_copy(inverse_ref, inverse, in_sem.at[0]),
        pltpu.make_async_copy(cross_ref, cross_in, in_sem.at[1]),
        pltpu.make_async_copy(lower_ref.at[:, y], local, in_sem.at[2]),
    )
    going = pltpu.make_async_copy(lower_ref.at[:, other], leaving, in_sem.at[3])
    going.start()
    for copy in inputs:
        copy.start()
    going.wait()
    pl.semaphore_wait(barrier, 3)
    cross_out(0)
    cross_out(1)
    stage_chunk(0)
    stage_chunk(1)
    for c in range(chunks):
        target_copy(c).start()

    for copy in inputs:
        copy.wait()
    left, right = inverse[0], inverse[1]
    joint = -matmul(matmul(right, cross_in[...], exact), left, exact)
    cross_in[...] = joint
    for index, matrix in enumerate((left, right, joint)):
        turned[index] = matrix.T
    mine = pl.ds(pl.multiple_of(y * share, 8), share)
    for index in range(2):
        turned_own[index] = inverse[index, mine, :].T
    turned_own[2] = cross_in[mine, :].T

    is_left = y == 0
    for dest, owner in enumerate((other, y)):
        theirs = pl.ds(pl.multiple_of(owner * share, 8), share)
        to_left, to_right, joined = (turned[index, theirs, :] for index in range(3))
        nothing = jnp.zeros_like(to_right)
        fold[dest, 0, 0] = jnp.where(is_left, nothing, to_right)
        fold[dest, 0, 1] = jnp.where(is_left, to_right, nothing)
        fold[dest, 1, 0] = jnp.where(is_left, to_left, joined)
        fold[dest, 1, 1] = jnp.where(is_left, joined, to_left)

    def buffer(group):
        return own_w if group == 2 else send_w.at[group]

    def gather_copy(group, kind, begin, count):
        spot = buffer(group).at[pl.ds(begin, count)]
        arrive = near_recv.at[group] if kind else far_recv.at[begin % pieces if group == 0 else pieces + group - 1]
        return pltpu.make_async_remote_copy(
            src_ref=spot,
            dst_ref=spot,
            send_sem=gather_send.at[group],
            recv_sem=arrive,
            device_id={"row": twin if kind else across},
            device_id_type=MESH,
        )

    def spread(group, i):
        gather_copy(group, 0, row * pieces + i, 1).start()
        gather_copy(group, 1, row * pieces + i, 1).start()

    def forward(group):
        if group == 0:

            def step(i, carry):
                settle(buffer(0).at[pl.ds(across * pieces + i, 1)], far_recv.at[i])
                gather_copy(0, 2, across * pieces + i, 1).start()
                return carry

            lax.fori_loop(0, pieces, step, 0)
        else:
            settle(buffer(group).at[pl.ds(across * pieces, pieces)], far_recv.at[pieces + group - 1])
            gather_copy(group, 2, across * pieces, pieces).start()

    def collect(group, held):
        settle(buffer(group).at[pl.ds((1 - core) * pieces, 2 * pieces)], near_recv.at[group])
        count = own_w.shape[1] if group == 2 else share
        for q in range(blocks):
            high, low = halves(buffer(group)[q])
            lanes = slice(q * width, (q + 1) * width)
            held[0:count, lanes] = high
            held[count : 2 * count, lanes] = low

    def convert(c):
        settle(stage.at[c % 2], stage_sem.at[c % 2])
        here = pl.ds(pl.multiple_of(c * chunk, chunk), chunk)
        for block in range(blocks):
            high, low = halves(stage[c % 2, block])
            lanes = slice(block * width, (block + 1) * width)
            trail_high[here, lanes] = high
            trail_low[here, lanes] = low

        @pl.when(c + 2 < chunks)
        def _():
            stage_chunk(c + 2)

    def summed(held, c):
        here = pl.ds(pl.multiple_of(c * chunk, chunk), chunk)
        count = held.shape[0] // 2
        both = contract_bf16(held[...], trail_high[here, :])
        return both[:count] + (both[count:] + contract_bf16(held[0:count, :], trail_low[here, :]))

    def begin(owner, group, c):
        theirs = pl.ds(pl.multiple_of(owner * share, 8), share)
        to_right = halves(target[c, share:panel, :])
        if group == 0:
            return three_pass(halves(turned_own[1, theirs, :]), to_right)
        to_left = halves(target[c, 0:share, :])
        return three_pass(halves(turned_own[0, theirs, :]), to_left) + three_pass(
            halves(turned_own[2, theirs, :]), to_right
        )

    def sum_copy(group, c):
        return pltpu.make_async_remote_copy(
            src_ref=sums_out.at[group, c],
            dst_ref=sums_in.at[group, c],
            send_sem=sum_send.at[0],
            recv_sem=sum_recv.at[1 + c // (chunks - 1) if group else 0],
            device_id={"col": other},
            device_id_type=MESH,
        )

    def share_out(group, c):
        sums_out[group, c] = begin(other, group, c) - summed(send_cat.at[group], c)
        sum_copy(group, c).start()

    def fold_right(i, _):
        settle(parcel.at[0, i], cross_recv.at[i])
        pair = parcel[0, i, height:share, :]
        crossed[i, :, rest:panel] = parcel[0, i, 0:height, :]
        crossed[i, low_rows, cut:rest] = turn(pair)
        crossed[i, high_rows, cut:rest] = pair
        send_w[0, row * pieces + i] = three_pass_last(fold[0, 0, 0], local[i]) + three_pass_last(
            fold[0, 0, 1, :, cut:panel], crossed[i, :, cut:panel]
        )
        spread(0, i)
        convert(i)
        return _

    lax.fori_loop(0, pieces, fold_right, 0)
    forward(0)
    collect(0, send_cat.at[0])
    settle(target, target_sem.at[0])

    def early(c, carry):
        share_out(0, c)

        @pl.when(c < chunks - pieces)
        def _():
            convert(c + pieces)

        return carry

    lax.fori_loop(0, chunks, early, 0)

    settle(parcel.at[1], cross_recv.at[pieces])

    def fold_left(i, _):
        pair, late_pair = parcel[0, i, height:share, :], parcel[1, i, height:share, :]
        crossed[i, :, 0:cut] = parcel[1, i, 0:height, :]
        crossed[i, low_rows, cut:rest] = jnp.where(is_low, late_pair, turn(pair))
        crossed[i, high_rows, cut:rest] = jnp.where(is_low, turn(late_pair), pair)
        send_w[1, row * pieces + i] = three_pass_last(fold[0, 1, 0], local[i]) + three_pass_last(
            fold[0, 1, 1], crossed[i]
        )
        spread(1, i)
        return _

    lax.fori_loop(0, pieces, fold_left, 0)

    def fold_own(i, _):
        for group in range(2):
            begins = (1 - group) * share
            own_w[row * pieces + i, begins : begins + share, :] = three_pass_last(
                fold[1, group, 0], local[i]
            ) + three_pass_last(fold[1, group, 1], crossed[i])
        spread(2, i)
        return _

    lax.fori_loop(0, pieces, fold_own, 0)
    forward(1)
    collect(1, send_cat.at[1])

    def late(c, _):
        share_out(1, c)
        return _

    lax.fori_loop(0, chunks, late, 0)
    forward(2)
    collect(2, own_cat)

    def mine_too(c, _):
        total = summed(own_cat, c)
        here = pl.ds(pl.multiple_of(c * chunk, chunk), chunk)
        out_ref[0:share, here] = begin(y, 1, c) - total[0:share]
        out_ref[share:panel, here] = begin(y, 0, c) - total[share:panel]
        return _

    lax.fori_loop(0, chunks, mine_too, 0)

    def finish(group, first, last):
        begins = (1 - group) * share

        def step(c, carry):
            here = pl.ds(pl.multiple_of(c * chunk, chunk), chunk)
            out_ref[begins : begins + share, here] += sums_in[group, c]
            return carry

        lax.fori_loop(first, last, step, 0)

    settle(sums_in.at[0], sum_recv.at[0])
    finish(0, 0, chunks)
    for group in range(3):
        settle(buffer(group).at[pl.ds(0, 3 * pieces)], gather_send.at[group])
    settle(packed, cross_send.at[0])
    settle(sums_in.at[1, pl.ds(0, chunks - 1)], sum_recv.at[1])
    finish(1, 0, chunks - 1)
    settle(sums_in.at[1, chunks - 1], sum_recv.at[2])
    finish(1, chunks - 1, chunks)
    settle(sums_out, sum_send.at[0])


def sweep(trailing, lower_trail, lower_cross, panel_inverse, target):
    rows, blocks, _, width = trailing.shape
    pieces, _, height, _ = lower_trail.shape
    panel = lower_cross.shape[0]
    share = panel // 2
    depth = blocks * width
    chunk = min(ROW_CHUNK, rows // 8)
    chunks = rows // chunk
    held = target.transpose(1, 2, 0).reshape(panel, rows)
    f32, bf16 = jnp.float32, jnp.bfloat16
    vmem, dma = pltpu.VMEM, pltpu.SemaphoreType.DMA
    out = pl.pallas_call(
        sweep_kernel,
        in_specs=[pl.BlockSpec(memory_space=pl.ANY)] * 5,
        out_specs=pl.BlockSpec(memory_space=pltpu.VMEM),
        out_shape=vmem((panel, rows), f32),
        scratch_shapes=[
            vmem((2, blocks, chunk, width), f32),
            vmem((rows, depth), bf16),
            vmem((rows, depth), bf16),
            vmem((pieces, height, panel), f32),
            vmem((pieces, height, panel), f32),
            vmem((2, pieces, share, LANES), f32),
            vmem((2, pieces, share, LANES), f32),
            vmem((pieces, height, panel), f32),
            vmem((2, panel, panel), f32),
            vmem((panel, panel), f32),
            vmem((chunks, panel, chunk), f32),
            vmem((3, panel, panel), f32),
            vmem((3, panel, share), f32),
            vmem((2, 2, 2, share, panel), f32),
            vmem((2, blocks, share, width), f32),
            vmem((blocks, panel, width), f32),
            vmem((2, panel, depth), bf16),
            vmem((2 * panel, depth), bf16),
            vmem((2, chunks, share, chunk), f32),
            vmem((2, chunks, share, chunk), f32),
            dma((2,)),
            dma((4,)),
            dma((1,)),
            dma((1,)),
            dma((pieces + 1,)),
            dma((3,)),
            dma((pieces + 2,)),
            dma((3,)),
            dma((1,)),
            dma((3,)),
        ],
        compiler_params=pltpu.CompilerParams(
            collective_id=0, has_side_effects=True, vmem_limit_bytes=58 * 1024 * 1024
        ),
    )(trailing.reshape(rows, blocks, width), lower_trail, lower_cross, panel_inverse, held)
    return out.reshape(2, share, rows).transpose(2, 0, 1)


def fits(trailing, lower_trail, lower_cross):
    rows, blocks, _, width = trailing.shape
    pieces, owners, height, held = lower_trail.shape
    panel = lower_cross.shape[0]
    return (
        lax.axis_size("row") == 4
        and lax.axis_size("col") == 2
        and owners == 2
        and held == panel
        and height == width == LANES
        and blocks == 4 * pieces
        and panel == 2 * (height + height // 2)
        and rows % (8 * LANES) == 0
        and rows // min(ROW_CHUNK, rows // 8) == 2 * pieces
    )


def per_device(trailing, lower_trail, lower_cross, panel_inverse, target):
    if fits(trailing, lower_trail, lower_cross):
        return sweep(trailing, lower_trail, lower_cross, panel_inverse, target)
    cols = lax.axis_size("col")
    me = lax.axis_index("col")
    rows, blocks, _, width = trailing.shape
    depth = lower_trail.shape[0] * width
    panel = lower_cross.shape[0]
    span = 2 * panel
    share = panel // cols
    out_cols = 2 * share
    held = span // cols

    def shift(array, step):
        if step == 0:
            return array
        return lax.ppermute(array, "col", [(i, (i + step) % cols) for i in range(cols)])

    pieces = []
    for step in range(cols):
        block = lax.dynamic_index_in_dim(lower_trail, (me + step) % cols, 1, keepdims=False)
        pieces.append(shift(block, step).reshape(depth, held))

    left, right = panel_inverse[0], panel_inverse[1]
    cross = matmul(matmul(right, lower_cross, exact), left, exact)
    top = jnp.concatenate([left.T, -cross.T], axis=1)
    bottom = jnp.concatenate([jnp.zeros_like(left), right.T], axis=1)
    by_owner = jnp.stack([top, bottom]).reshape(2, cols, share, span)

    def owner_fold(owner):
        return lax.dynamic_index_in_dim(by_owner, owner, 1, keepdims=False).reshape(out_cols, span)

    def gathered(fold, part):
        total = None
        for back, piece in enumerate(pieces):
            source = (me - back) % cols
            weights = lax.dynamic_slice_in_dim(fold[part], source * held, held, 1)
            term = contract_last(piece, weights)
            total = term if total is None else total + term
        return lax.all_gather(total, "row", axis=0, tiled=True)

    held_col = jnp.arange(out_cols)
    place = (held_col // share) * panel + me * share + held_col % share
    pick = (place[:, None] == jnp.arange(span)[None, :]).astype(jnp.float32)

    trail = trailing.reshape(rows, blocks, width)
    own_target = target.transpose(1, 2, 0).reshape(out_cols, rows)
    first = LANES if out_cols > LANES else out_cols
    parts = [slice(0, first)] + ([slice(first, out_cols)] if first < out_cols else [])
    folds = [owner_fold((me + step) % cols) for step in range(cols)]
    factors = {}
    for step in range(1, cols):
        for index, part in enumerate(parts):
            factors[step, index] = gathered(folds[step], part)
    own_factor = gathered(folds[0], slice(0, out_cols))

    chunks = CHUNKS if rows % (CHUNKS * LANES) == 0 else 1
    arrived = [[[] for _ in range(chunks)] for _ in parts]
    for step in range(1, cols):
        weights = contract_last(folds[step], pick, exact)
        for index, part in enumerate(parts):
            for chunk in range(chunks):
                partial = share_of(trail, factors[step, index], weights[part], own_target, chunk, chunks)
                arrived[index][chunk].append(shift(partial, step))
    own = share_of(trail, own_factor, contract_last(folds[0], pick, exact), own_target)
    if cols == 1:
        return own.reshape(2, share, rows).transpose(2, 0, 1)
    others = []
    for pieces_here in arrived:
        sums = [sum(group[1:], group[0]) for group in pieces_here]
        others.append(jnp.concatenate(sums, axis=1))
    result = own + jnp.concatenate(others, axis=0)
    return result.reshape(2, share, rows).transpose(2, 0, 1)


def solution(mesh):
    placed = (
        P(("copy", "row"), None, "col", None),
        P(("copy", "row"), None, None, "col"),
        P(),
        P(),
        P(("copy", "row"), None, "col"),
    )
    return jax.shard_map(
        per_device,
        mesh=mesh,
        in_specs=placed,
        out_specs=P(("copy", "row"), None, "col"),
        check_vma=False,
    )
```

```python
import jax
import jax.numpy as jnp
from jax import lax
from jax.experimental import pallas as pl
from jax.experimental.pallas import tpu as pltpu
from jax.sharding import PartitionSpec as P

ROW_TILE = 256
LANES = 128
CHUNKS = 2
exact = lax.Precision.HIGHEST


def matmul(first, second, precision=lax.Precision.HIGH):
    return jnp.dot(first, second, preferred_element_type=jnp.float32, precision=precision)


def contract_last(first, second, precision=lax.Precision.HIGH):
    return lax.dot_general(
        first, second, (((1,), (1,)), ((), ())), preferred_element_type=jnp.float32, precision=precision
    )


def halves(value):
    high = value.astype(jnp.bfloat16)
    return high, (value - high.astype(jnp.float32)).astype(jnp.bfloat16)


def three_pass(first, second):
    first_high, first_low = first
    second_high, second_low = second

    def product(a, b):
        return jnp.dot(a, b, preferred_element_type=jnp.float32)

    return product(first_high, second_high) + (product(first_high, second_low) + product(first_low, second_high))


def share_kernel(trail_ref, factor_ref, weight_ref, target_ref, out_ref, high_ref, low_ref):
    @pl.when(pl.program_id(0) == 0)
    def _():
        high_ref[...], low_ref[...] = halves(factor_ref[...])

    blocks = trail_ref.shape[1]
    trail = jnp.concatenate([trail_ref[:, block, :] for block in range(blocks)], axis=1)
    summed = three_pass(halves(trail), (high_ref[...], low_ref[...]))
    start = three_pass(halves(weight_ref[...]), halves(target_ref[...]))
    out_ref[...] = start - summed.T


def share_of(trail, factor, weight, target, chunk=0, chunks=1):
    rows, blocks, width = trail.shape
    depth, out_cols = factor.shape
    in_cols = target.shape[0]
    count = rows // chunks
    tile = min(ROW_TILE, count)
    begin = chunk * (count // tile)
    return pl.pallas_call(
        share_kernel,
        grid=(count // tile,),
        in_specs=[
            pl.BlockSpec((tile, blocks, width), lambda i: (i + begin, 0, 0)),
            pl.BlockSpec((depth, out_cols), lambda i: (0, 0)),
            pl.BlockSpec((out_cols, in_cols), lambda i: (0, 0)),
            pl.BlockSpec((in_cols, tile), lambda i: (0, i + begin)),
        ],
        out_specs=pl.BlockSpec((out_cols, tile), lambda i: (0, i)),
        out_shape=jax.ShapeDtypeStruct((out_cols, count), jnp.float32),
        scratch_shapes=[pltpu.VMEM((depth, out_cols), jnp.bfloat16)] * 2,
        compiler_params=pltpu.CompilerParams(dimension_semantics=("arbitrary",)),
        cost_estimate=pl.CostEstimate(
            flops=6 * count * depth * out_cols, bytes_accessed=4 * count * depth, transcendentals=0
        ),
    )(trail, factor, weight, target)


MESH = pl.DeviceIdType.MESH
ROW_CHUNK = 256


def contract_bf16(first, second):
    return lax.dot_general(first, second, (((1,), (1,)), ((), ())), preferred_element_type=jnp.float32)


def three_pass_last(first, second):
    first_high, first_low = halves(first)
    second_high, second_low = halves(second)
    return contract_bf16(first_high, second_high) + (
        contract_bf16(first_high, second_low) + contract_bf16(first_low, second_high)
    )


def sweep_kernel(
    trail_ref, lower_ref, cross_ref, inverse_ref, target_ref, out_ref,
    stage, trail_high, trail_low, local, leaving, packed, parcel, crossed, inverse, cross_in, target, turned, turned_own, fold,
    send_w, own_w, send_cat, own_cat, sums_out, sums_in,
    stage_sem, in_sem, target_sem, cross_send, cross_recv, gather_send, far_recv, near_recv, sum_send, sum_recv,
):
    row = lax.axis_index("row")
    y = lax.axis_index("col")
    chip, core = row // 2, row % 2
    across = (1 - chip) * 2 + core
    twin = chip * 2 + (1 - core)
    across_twin = (1 - chip) * 2 + (1 - core)
    other = 1 - y
    pieces, height, panel = local.shape
    share = panel // 2
    rows, blocks, width = trail_ref.shape
    chunk = stage.shape[2]
    chunks = rows // chunk
    cut = share // LANES * LANES
    rest = cut + LANES
    odd = share - cut
    low_rows, high_rows = slice(0, height // 2), slice(height // 2, height)
    is_low = lax.broadcasted_iota(jnp.int32, (height // 2, LANES), 1) < odd

    barrier = pltpu.get_barrier_semaphore()
    for place in ({"col": other}, {"row": across}, {"row": twin}):
        pl.semaphore_signal(barrier, inc=1, device_id=place, device_id_type=MESH)

    def settle(ref, sem):
        pltpu.make_async_copy(ref, ref, sem).wait()

    def turn(value):
        return pltpu.roll(value, odd, 1)

    def cross_copy(part, i):
        return pltpu.make_async_remote_copy(
            src_ref=packed.at[part, i],
            dst_ref=parcel.at[part, i],
            send_sem=cross_send.at[0],
            recv_sem=cross_recv.at[i if part == 0 else pieces],
            device_id={"col": other},
            device_id_type=MESH,
        )

    def cross_out(part):
        def step(i, carry):
            upper = leaving[i, low_rows, cut:rest]
            lower = leaving[i, high_rows, cut:rest]
            if part == 0:
                packed[0, i, 0:height, :] = leaving[i, :, rest:panel]
                packed[0, i, height:share, :] = jnp.where(is_low, turn(upper), lower)
            else:
                packed[1, i, 0:height, :] = leaving[i, :, 0:cut]
                packed[1, i, height:share, :] = jnp.where(is_low, upper, turn(lower))
            cross_copy(part, i).start()
            return carry

        lax.fori_loop(0, pieces, step, 0)

    def stage_copy(c, block):
        return pltpu.make_async_copy(
            trail_ref.at[pl.ds(c * chunk, chunk), block], stage.at[c % 2, block], stage_sem.at[c % 2]
        )

    def stage_chunk(c):
        for block in range(blocks):
            stage_copy(c, block).start()

    def target_copy(c):
        return pltpu.make_async_copy(
            target_ref.at[:, pl.ds(pl.multiple_of(c * chunk, chunk), chunk)], target.at[c], target_sem.at[0]
        )

    inputs = (
        pltpu.make_async_copy(inverse_ref, inverse, in_sem.at[0]),
        pltpu.make_async_copy(cross_ref, cross_in, in_sem.at[1]),
        pltpu.make_async_copy(lower_ref.at[:, y], local, in_sem.at[2]),
    )
    going = pltpu.make_async_copy(lower_ref.at[:, other], leaving, in_sem.at[3])
    going.start()
    for copy in inputs:
        copy.start()
    going.wait()
    pl.semaphore_wait(barrier, 3)
    cross_out(0)
    cross_out(1)
    stage_chunk(0)
    stage_chunk(1)
    for c in range(chunks):
        target_copy(c).start()

    for copy in inputs:
        copy.wait()
    left, right = inverse[0], inverse[1]
    joint = -matmul(matmul(right, cross_in[...], exact), left, exact)
    cross_in[...] = joint
    for index, matrix in enumerate((left, right, joint)):
        turned[index] = matrix.T
    mine = pl.ds(pl.multiple_of(y * share, 8), share)
    for index in range(2):
        turned_own[index] = inverse[index, mine, :].T
    turned_own[2] = cross_in[mine, :].T

    is_left = y == 0
    for dest, owner in enumerate((other, y)):
        theirs = pl.ds(pl.multiple_of(owner * share, 8), share)
        to_left, to_right, joined = (turned[index, theirs, :] for index in range(3))
        nothing = jnp.zeros_like(to_right)
        fold[dest, 0, 0] = jnp.where(is_left, nothing, to_right)
        fold[dest, 0, 1] = jnp.where(is_left, to_right, nothing)
        fold[dest, 1, 0] = jnp.where(is_left, to_left, joined)
        fold[dest, 1, 1] = jnp.where(is_left, joined, to_left)

    def buffer(group):
        return own_w if group == 2 else send_w.at[group]

    def gather_copy(group, kind, begin, count):
        spot = buffer(group).at[pl.ds(begin, count)]
        if group:
            far, near = pieces + group - 1, group
        else:
            far, near = begin % pieces, begin % pieces // (pieces - 1) * 3
        arrive = near_recv.at[near] if kind else far_recv.at[far]
        return pltpu.make_async_remote_copy(
            src_ref=spot,
            dst_ref=spot,
            send_sem=gather_send.at[group],
            recv_sem=arrive,
            device_id={"row": twin if kind else across},
            device_id_type=MESH,
        )

    def spread(group, i):
        gather_copy(group, 0, row * pieces + i, 1).start()
        gather_copy(group, 1, row * pieces + i, 1).start()

    def forward(group):
        settle(buffer(group).at[pl.ds(across * pieces, pieces)], far_recv.at[pieces + group - 1])
        gather_copy(group, 2, across * pieces, pieces).start()

    def forward_right(first, last):
        def step(i, carry):
            settle(buffer(0).at[pl.ds(across * pieces + i, 1)], far_recv.at[i])
            gather_copy(0, 2, across * pieces + i, 1).start()
            return carry

        lax.fori_loop(first, last, step, 0)

    def lanes_of(q):
        place = q % pieces * (blocks // pieces) + q // pieces
        return slice(place * width, (place + 1) * width)

    def split(group, held, chosen):
        count = own_w.shape[1] if group == 2 else share
        for q in chosen:
            high, low = halves(buffer(group)[q])
            held[0:count, lanes_of(q)] = high
            held[count : 2 * count, lanes_of(q)] = low

    def collect(group, held):
        settle(buffer(group).at[pl.ds((1 - core) * pieces, 2 * pieces)], near_recv.at[group])
        split(group, held, range(blocks))

    def convert(c):
        settle(stage.at[c % 2], stage_sem.at[c % 2])
        here = pl.ds(pl.multiple_of(c * chunk, chunk), chunk)
        for block in range(blocks):
            high, low = halves(stage[c % 2, block])
            trail_high[here, lanes_of(block)] = high
            trail_low[here, lanes_of(block)] = low

        @pl.when(c + 2 < chunks)
        def _():
            stage_chunk(c + 2)

    def summed(held, c, part=slice(None)):
        here = pl.ds(pl.multiple_of(c * chunk, chunk), chunk)
        count = held.shape[0] // 2
        both = contract_bf16(held[:, part], trail_high[here, part])
        return both[:count] + (both[count:] + contract_bf16(held[0:count, part], trail_low[here, part]))

    def begin(owner, group, c):
        theirs = pl.ds(pl.multiple_of(owner * share, 8), share)
        to_right = halves(target[c, share:panel, :])
        if group == 0:
            return three_pass(halves(turned_own[1, theirs, :]), to_right)
        to_left = halves(target[c, 0:share, :])
        return three_pass(halves(turned_own[0, theirs, :]), to_left) + three_pass(
            halves(turned_own[2, theirs, :]), to_right
        )

    def sum_copy(group, c):
        return pltpu.make_async_remote_copy(
            src_ref=sums_out.at[group, c],
            dst_ref=sums_in.at[group, c],
            send_sem=sum_send.at[0],
            recv_sem=sum_recv.at[1 + c // (chunks - 1) if group else 0],
            device_id={"col": other},
            device_id_type=MESH,
        )

    def share_out(group, c):
        sums_out[group, c] = begin(other, group, c) - summed(send_cat.at[group], c)
        sum_copy(group, c).start()

    def fold_right(i, _):
        settle(parcel.at[0, i], cross_recv.at[i])
        pair = parcel[0, i, height:share, :]
        crossed[i, :, rest:panel] = parcel[0, i, 0:height, :]
        crossed[i, low_rows, cut:rest] = turn(pair)
        crossed[i, high_rows, cut:rest] = pair
        send_w[0, row * pieces + i] = three_pass_last(fold[0, 0, 0], local[i]) + three_pass_last(
            fold[0, 0, 1, :, cut:panel], crossed[i, :, cut:panel]
        )
        spread(0, i)
        convert(i)
        return _

    lax.fori_loop(0, pieces, fold_right, 0)
    last = pieces - 1
    mark = last * (blocks // pieces) * width
    settle(target, target_sem.at[0])
    forward_right(0, last)

    @pl.when(core == 1)
    def _():
        forward_right(last, pieces)

    settle(buffer(0).at[pl.ds(0, 2 * last)], near_recv.at[0])
    split(0, send_cat.at[0], [q for q in range(blocks) if q % pieces < last])
    sums_out[0, 0] = begin(other, 0, 0) - summed(send_cat.at[0], 0, slice(0, mark))

    @pl.when(core == 0)
    def _():
        forward_right(last, pieces)

    settle(buffer(0).at[pl.ds(0, 2)], near_recv.at[3])
    split(0, send_cat.at[0], [q for q in range(blocks) if q % pieces == last])
    sums_out[0, 0] -= summed(send_cat.at[0], 0, slice(mark, None))
    sum_copy(0, 0).start()
    convert(pieces)

    def early(c, carry):
        share_out(0, c)

        @pl.when(c < chunks - pieces)
        def _():
            convert(c + pieces)

        return carry

    lax.fori_loop(1, chunks, early, 0)

    settle(parcel.at[1], cross_recv.at[pieces])

    def fold_left(i, _):
        pair, late_pair = parcel[0, i, height:share, :], parcel[1, i, height:share, :]
        crossed[i, :, 0:cut] = parcel[1, i, 0:height, :]
        crossed[i, low_rows, cut:rest] = jnp.where(is_low, late_pair, turn(pair))
        crossed[i, high_rows, cut:rest] = jnp.where(is_low, turn(late_pair), pair)
        send_w[1, row * pieces + i] = three_pass_last(fold[0, 1, 0], local[i]) + three_pass_last(
            fold[0, 1, 1], crossed[i]
        )
        spread(1, i)
        return _

    lax.fori_loop(0, pieces, fold_left, 0)

    def fold_own(i, _):
        for group in range(2):
            begins = (1 - group) * share
            own_w[row * pieces + i, begins : begins + share, :] = three_pass_last(
                fold[1, group, 0], local[i]
            ) + three_pass_last(fold[1, group, 1], crossed[i])
        spread(2, i)
        return _

    lax.fori_loop(0, pieces, fold_own, 0)
    forward(1)
    collect(1, send_cat.at[1])

    def late(c, _):
        share_out(1, c)
        return _

    lax.fori_loop(0, chunks, late, 0)
    forward(2)
    collect(2, own_cat)

    def mine_too(c, _):
        total = summed(own_cat, c)
        here = pl.ds(pl.multiple_of(c * chunk, chunk), chunk)
        out_ref[0:share, here] = begin(y, 1, c) - total[0:share]
        out_ref[share:panel, here] = begin(y, 0, c) - total[share:panel]
        return _

    lax.fori_loop(0, chunks, mine_too, 0)

    def finish(group, first, last):
        begins = (1 - group) * share

        def step(c, carry):
            here = pl.ds(pl.multiple_of(c * chunk, chunk), chunk)
            out_ref[begins : begins + share, here] += sums_in[group, c]
            return carry

        lax.fori_loop(first, last, step, 0)

    settle(sums_in.at[0], sum_recv.at[0])
    finish(0, 0, chunks)
    for group in range(3):
        settle(buffer(group).at[pl.ds(0, 3 * pieces)], gather_send.at[group])
    settle(packed, cross_send.at[0])
    settle(sums_in.at[1, pl.ds(0, chunks - 1)], sum_recv.at[1])
    finish(1, 0, chunks - 1)
    settle(sums_in.at[1, chunks - 1], sum_recv.at[2])
    finish(1, chunks - 1, chunks)
    settle(sums_out, sum_send.at[0])


def sweep(trailing, lower_trail, lower_cross, panel_inverse, target):
    rows, blocks, _, width = trailing.shape
    pieces, _, height, _ = lower_trail.shape
    panel = lower_cross.shape[0]
    share = panel // 2
    depth = blocks * width
    chunk = min(ROW_CHUNK, rows // 8)
    chunks = rows // chunk
    held = target.transpose(1, 2, 0).reshape(panel, rows)
    f32, bf16 = jnp.float32, jnp.bfloat16
    vmem, dma = pltpu.VMEM, pltpu.SemaphoreType.DMA
    out = pl.pallas_call(
        sweep_kernel,
        in_specs=[pl.BlockSpec(memory_space=pl.ANY)] * 5,
        out_specs=pl.BlockSpec(memory_space=pltpu.VMEM),
        out_shape=vmem((panel, rows), f32),
        scratch_shapes=[
            vmem((2, blocks, chunk, width), f32),
            vmem((rows, depth), bf16),
            vmem((rows, depth), bf16),
            vmem((pieces, height, panel), f32),
            vmem((pieces, height, panel), f32),
            vmem((2, pieces, share, LANES), f32),
            vmem((2, pieces, share, LANES), f32),
            vmem((pieces, height, panel), f32),
            vmem((2, panel, panel), f32),
            vmem((panel, panel), f32),
            vmem((chunks, panel, chunk), f32),
            vmem((3, panel, panel), f32),
            vmem((3, panel, share), f32),
            vmem((2, 2, 2, share, panel), f32),
            vmem((2, blocks, share, width), f32),
            vmem((blocks, panel, width), f32),
            vmem((2, panel, depth), bf16),
            vmem((2 * panel, depth), bf16),
            vmem((2, chunks, share, chunk), f32),
            vmem((2, chunks, share, chunk), f32),
            dma((2,)),
            dma((4,)),
            dma((1,)),
            dma((1,)),
            dma((pieces + 1,)),
            dma((3,)),
            dma((pieces + 2,)),
            dma((4,)),
            dma((1,)),
            dma((3,)),
        ],
        compiler_params=pltpu.CompilerParams(
            collective_id=0, has_side_effects=True, vmem_limit_bytes=58 * 1024 * 1024
        ),
    )(trailing.reshape(rows, blocks, width), lower_trail, lower_cross, panel_inverse, held)
    return out.reshape(2, share, rows).transpose(2, 0, 1)


def fits(trailing, lower_trail, lower_cross):
    rows, blocks, _, width = trailing.shape
    pieces, owners, height, held = lower_trail.shape
    panel = lower_cross.shape[0]
    return (
        lax.axis_size("row") == 4
        and lax.axis_size("col") == 2
        and owners == 2
        and held == panel
        and height == width == LANES
        and blocks == 4 * pieces
        and panel == 2 * (height + height // 2)
        and rows % (8 * LANES) == 0
        and rows // min(ROW_CHUNK, rows // 8) == 2 * pieces
    )


def per_device(trailing, lower_trail, lower_cross, panel_inverse, target):
    if fits(trailing, lower_trail, lower_cross):
        return sweep(trailing, lower_trail, lower_cross, panel_inverse, target)
    cols = lax.axis_size("col")
    me = lax.axis_index("col")
    rows, blocks, _, width = trailing.shape
    depth = lower_trail.shape[0] * width
    panel = lower_cross.shape[0]
    span = 2 * panel
    share = panel // cols
    out_cols = 2 * share
    held = span // cols

    def shift(array, step):
        if step == 0:
            return array
        return lax.ppermute(array, "col", [(i, (i + step) % cols) for i in range(cols)])

    pieces = []
    for step in range(cols):
        block = lax.dynamic_index_in_dim(lower_trail, (me + step) % cols, 1, keepdims=False)
        pieces.append(shift(block, step).reshape(depth, held))

    left, right = panel_inverse[0], panel_inverse[1]
    cross = matmul(matmul(right, lower_cross, exact), left, exact)
    top = jnp.concatenate([left.T, -cross.T], axis=1)
    bottom = jnp.concatenate([jnp.zeros_like(left), right.T], axis=1)
    by_owner = jnp.stack([top, bottom]).reshape(2, cols, share, span)

    def owner_fold(owner):
        return lax.dynamic_index_in_dim(by_owner, owner, 1, keepdims=False).reshape(out_cols, span)

    def gathered(fold, part):
        total = None
        for back, piece in enumerate(pieces):
            source = (me - back) % cols
            weights = lax.dynamic_slice_in_dim(fold[part], source * held, held, 1)
            term = contract_last(piece, weights)
            total = term if total is None else total + term
        return lax.all_gather(total, "row", axis=0, tiled=True)

    held_col = jnp.arange(out_cols)
    place = (held_col // share) * panel + me * share + held_col % share
    pick = (place[:, None] == jnp.arange(span)[None, :]).astype(jnp.float32)

    trail = trailing.reshape(rows, blocks, width)
    own_target = target.transpose(1, 2, 0).reshape(out_cols, rows)
    first = LANES if out_cols > LANES else out_cols
    parts = [slice(0, first)] + ([slice(first, out_cols)] if first < out_cols else [])
    folds = [owner_fold((me + step) % cols) for step in range(cols)]
    factors = {}
    for step in range(1, cols):
        for index, part in enumerate(parts):
            factors[step, index] = gathered(folds[step], part)
    own_factor = gathered(folds[0], slice(0, out_cols))

    chunks = CHUNKS if rows % (CHUNKS * LANES) == 0 else 1
    arrived = [[[] for _ in range(chunks)] for _ in parts]
    for step in range(1, cols):
        weights = contract_last(folds[step], pick, exact)
        for index, part in enumerate(parts):
            for chunk in range(chunks):
                partial = share_of(trail, factors[step, index], weights[part], own_target, chunk, chunks)
                arrived[index][chunk].append(shift(partial, step))
    own = share_of(trail, own_factor, contract_last(folds[0], pick, exact), own_target)
    if cols == 1:
        return own.reshape(2, share, rows).transpose(2, 0, 1)
    others = []
    for pieces_here in arrived:
        sums = [sum(group[1:], group[0]) for group in pieces_here]
        others.append(jnp.concatenate(sums, axis=1))
    result = own + jnp.concatenate(others, axis=0)
    return result.reshape(2, share, rows).transpose(2, 0, 1)


def solution(mesh):
    placed = (
        P(("copy", "row"), None, "col", None),
        P(("copy", "row"), None, None, "col"),
        P(),
        P(),
        P(("copy", "row"), None, "col"),
    )
    return jax.shard_map(
        per_device,
        mesh=mesh,
        in_specs=placed,
        out_specs=P(("copy", "row"), None, "col"),
        check_vma=False,
    )
```

```python
import jax
import jax.numpy as jnp
from jax import lax
from jax.experimental import pallas as pl
from jax.experimental.pallas import tpu as pltpu
from jax.sharding import PartitionSpec as P

ROW_TILE = 256
LANES = 128
CHUNKS = 2
exact = lax.Precision.HIGHEST


def matmul(first, second, precision=lax.Precision.HIGH):
    return jnp.dot(first, second, preferred_element_type=jnp.float32, precision=precision)


def contract_last(first, second, precision=lax.Precision.HIGH):
    return lax.dot_general(
        first, second, (((1,), (1,)), ((), ())), preferred_element_type=jnp.float32, precision=precision
    )


def halves(value):
    high = value.astype(jnp.bfloat16)
    return high, (value - high.astype(jnp.float32)).astype(jnp.bfloat16)


def three_pass(first, second):
    first_high, first_low = first
    second_high, second_low = second

    def product(a, b):
        return jnp.dot(a, b, preferred_element_type=jnp.float32)

    return product(first_high, second_high) + (product(first_high, second_low) + product(first_low, second_high))


def share_kernel(trail_ref, factor_ref, weight_ref, target_ref, out_ref, high_ref, low_ref):
    @pl.when(pl.program_id(0) == 0)
    def _():
        high_ref[...], low_ref[...] = halves(factor_ref[...])

    blocks = trail_ref.shape[1]
    trail = jnp.concatenate([trail_ref[:, block, :] for block in range(blocks)], axis=1)
    summed = three_pass(halves(trail), (high_ref[...], low_ref[...]))
    start = three_pass(halves(weight_ref[...]), halves(target_ref[...]))
    out_ref[...] = start - summed.T


def share_of(trail, factor, weight, target, chunk=0, chunks=1):
    rows, blocks, width = trail.shape
    depth, out_cols = factor.shape
    in_cols = target.shape[0]
    count = rows // chunks
    tile = min(ROW_TILE, count)
    begin = chunk * (count // tile)
    return pl.pallas_call(
        share_kernel,
        grid=(count // tile,),
        in_specs=[
            pl.BlockSpec((tile, blocks, width), lambda i: (i + begin, 0, 0)),
            pl.BlockSpec((depth, out_cols), lambda i: (0, 0)),
            pl.BlockSpec((out_cols, in_cols), lambda i: (0, 0)),
            pl.BlockSpec((in_cols, tile), lambda i: (0, i + begin)),
        ],
        out_specs=pl.BlockSpec((out_cols, tile), lambda i: (0, i)),
        out_shape=jax.ShapeDtypeStruct((out_cols, count), jnp.float32),
        scratch_shapes=[pltpu.VMEM((depth, out_cols), jnp.bfloat16)] * 2,
        compiler_params=pltpu.CompilerParams(dimension_semantics=("arbitrary",)),
        cost_estimate=pl.CostEstimate(
            flops=6 * count * depth * out_cols, bytes_accessed=4 * count * depth, transcendentals=0
        ),
    )(trail, factor, weight, target)


MESH = pl.DeviceIdType.MESH
ROW_CHUNK = 256


def contract_bf16(first, second):
    return lax.dot_general(first, second, (((1,), (1,)), ((), ())), preferred_element_type=jnp.float32)


def three_pass_last(first, second):
    first_high, first_low = halves(first)
    second_high, second_low = halves(second)
    return contract_bf16(first_high, second_high) + (
        contract_bf16(first_high, second_low) + contract_bf16(first_low, second_high)
    )


def sweep_kernel(
    trail_ref, lower_ref, cross_ref, inverse_ref, target_ref, out_ref,
    stage, trail_high, trail_low, local, leaving, packed, parcel, crossed, inverse, cross_in, target, turned, turned_own, fold,
    send_w, own_w, send_cat, own_cat, sums_out, sums_in,
    stage_sem, in_sem, target_sem, cross_send, cross_recv, gather_send, far_recv, near_recv, sum_send, sum_recv,
):
    row = lax.axis_index("row")
    y = lax.axis_index("col")
    chip, core = row // 2, row % 2
    across = (1 - chip) * 2 + core
    twin = chip * 2 + (1 - core)
    across_twin = (1 - chip) * 2 + (1 - core)
    other = 1 - y
    pieces, height, panel = local.shape
    share = panel // 2
    rows, blocks, width = trail_ref.shape
    chunk = stage.shape[2]
    chunks = rows // chunk
    cut = share // LANES * LANES
    rest = cut + LANES
    odd = share - cut
    low_rows, high_rows = slice(0, height // 2), slice(height // 2, height)
    is_low = lax.broadcasted_iota(jnp.int32, (height // 2, LANES), 1) < odd

    barrier = pltpu.get_barrier_semaphore()
    for place in ({"col": other}, {"row": across}, {"row": twin}):
        pl.semaphore_signal(barrier, inc=1, device_id=place, device_id_type=MESH)

    def settle(ref, sem):
        pltpu.make_async_copy(ref, ref, sem).wait()

    def turn(value):
        return pltpu.roll(value, odd, 1)

    def cross_copy(part, i):
        return pltpu.make_async_remote_copy(
            src_ref=packed.at[part, i],
            dst_ref=parcel.at[part, i],
            send_sem=cross_send.at[0],
            recv_sem=cross_recv.at[i if part == 0 else pieces],
            device_id={"col": other},
            device_id_type=MESH,
        )

    def pack(part, i):
        upper = leaving[i, low_rows, cut:rest]
        lower = leaving[i, high_rows, cut:rest]
        if part == 0:
            packed[0, i, 0:height, :] = leaving[i, :, rest:panel]
            packed[0, i, height:share, :] = jnp.where(is_low, turn(upper), lower)
        else:
            packed[1, i, 0:height, :] = leaving[i, :, 0:cut]
            packed[1, i, height:share, :] = jnp.where(is_low, upper, turn(lower))

    def cross_out(part, first):
        def step(i, carry):
            pack(part, i)
            cross_copy(part, i).start()
            return carry

        lax.fori_loop(first, pieces, step, 0)

    def stage_copy(c, block):
        return pltpu.make_async_copy(
            trail_ref.at[pl.ds(c * chunk, chunk), block], stage.at[c % 2, block], stage_sem.at[c % 2]
        )

    def stage_chunk(c):
        for block in range(blocks):
            stage_copy(c, block).start()

    def target_copy(c):
        return pltpu.make_async_copy(
            target_ref.at[:, pl.ds(pl.multiple_of(c * chunk, chunk), chunk)], target.at[c], target_sem.at[0]
        )

    inputs = (
        pltpu.make_async_copy(inverse_ref, inverse, in_sem.at[0]),
        pltpu.make_async_copy(cross_ref, cross_in, in_sem.at[1]),
        pltpu.make_async_copy(lower_ref.at[:, y], local, in_sem.at[2]),
    )
    going = pltpu.make_async_copy(lower_ref.at[:, other], leaving, in_sem.at[3])
    going.start()
    for copy in inputs:
        copy.start()
    going.wait()
    pack(0, 0)
    pl.semaphore_wait(barrier, 3)
    cross_copy(0, 0).start()
    cross_out(0, 1)
    cross_out(1, 0)
    stage_chunk(0)
    stage_chunk(1)
    for c in range(chunks):
        target_copy(c).start()

    for copy in inputs:
        copy.wait()
    left, right = inverse[0], inverse[1]
    joint = -matmul(matmul(right, cross_in[...], exact), left, exact)
    cross_in[...] = joint
    for index, matrix in enumerate((left, right, joint)):
        turned[index] = matrix.T
    mine = pl.ds(pl.multiple_of(y * share, 8), share)
    for index in range(2):
        turned_own[index] = inverse[index, mine, :].T
    turned_own[2] = cross_in[mine, :].T

    is_left = y == 0
    for dest, owner in enumerate((other, y)):
        theirs = pl.ds(pl.multiple_of(owner * share, 8), share)
        to_left, to_right, joined = (turned[index, theirs, :] for index in range(3))
        nothing = jnp.zeros_like(to_right)
        fold[dest, 0, 0] = jnp.where(is_left, nothing, to_right)
        fold[dest, 0, 1] = jnp.where(is_left, to_right, nothing)
        fold[dest, 1, 0] = jnp.where(is_left, to_left, joined)
        fold[dest, 1, 1] = jnp.where(is_left, joined, to_left)

    def buffer(group):
        return own_w if group == 2 else send_w.at[group]

    def gather_copy(group, kind, begin, count):
        spot = buffer(group).at[pl.ds(begin, count)]
        if group:
            far, near = pieces + group - 1, group
        else:
            far, near = begin % pieces, begin % pieces // (pieces - 1) * 3
        arrive = near_recv.at[near] if kind else far_recv.at[far]
        return pltpu.make_async_remote_copy(
            src_ref=spot,
            dst_ref=spot,
            send_sem=gather_send.at[group // 2],
            recv_sem=arrive,
            device_id={"row": twin if kind else across},
            device_id_type=MESH,
        )

    def spread(group, i):
        gather_copy(group, 0, row * pieces + i, 1).start()
        gather_copy(group, 1, row * pieces + i, 1).start()

    def forward(group):
        settle(buffer(group).at[pl.ds(across * pieces, pieces)], far_recv.at[pieces + group - 1])
        gather_copy(group, 2, across * pieces, pieces).start()

    def forward_right(first, last):
        def step(i, carry):
            settle(buffer(0).at[pl.ds(across * pieces + i, 1)], far_recv.at[i])
            gather_copy(0, 2, across * pieces + i, 1).start()
            return carry

        lax.fori_loop(first, last, step, 0)

    def lanes_of(q):
        place = q % pieces * (blocks // pieces) + q // pieces
        return slice(place * width, (place + 1) * width)

    def split(group, held, chosen):
        count = own_w.shape[1] if group == 2 else share
        for q in chosen:
            high, low = halves(buffer(group)[q])
            held[0:count, lanes_of(q)] = high
            held[count : 2 * count, lanes_of(q)] = low

    def collect(group, held):
        settle(buffer(group).at[pl.ds((1 - core) * pieces, 2 * pieces)], near_recv.at[group])
        split(group, held, range(blocks))

    def convert(c):
        settle(stage.at[c % 2], stage_sem.at[c % 2])
        here = pl.ds(pl.multiple_of(c * chunk, chunk), chunk)
        for block in range(blocks):
            high, low = halves(stage[c % 2, block])
            trail_high[here, lanes_of(block)] = high
            trail_low[here, lanes_of(block)] = low

        @pl.when(c + 2 < chunks)
        def _():
            stage_chunk(c + 2)

    def summed(held, c, part=slice(None)):
        here = pl.ds(pl.multiple_of(c * chunk, chunk), chunk)
        count = held.shape[0] // 2
        both = contract_bf16(held[:, part], trail_high[here, part])
        return both[:count] + (both[count:] + contract_bf16(held[0:count, part], trail_low[here, part]))

    def begin(owner, group, c):
        theirs = pl.ds(pl.multiple_of(owner * share, 8), share)
        to_right = halves(target[c, share:panel, :])
        if group == 0:
            return three_pass(halves(turned_own[1, theirs, :]), to_right)
        to_left = halves(target[c, 0:share, :])
        return three_pass(halves(turned_own[0, theirs, :]), to_left) + three_pass(
            halves(turned_own[2, theirs, :]), to_right
        )

    def sum_copy(group, c):
        return pltpu.make_async_remote_copy(
            src_ref=sums_out.at[group, c],
            dst_ref=sums_in.at[group, c],
            send_sem=sum_send.at[0],
            recv_sem=sum_recv.at[1 + c // (chunks - 1) if group else 0],
            device_id={"col": other},
            device_id_type=MESH,
        )

    def share_out(group, c):
        sums_out[group, c] = begin(other, group, c) - summed(send_cat.at[group], c)
        sum_copy(group, c).start()

    def fold_right(i, _):
        settle(parcel.at[0, i], cross_recv.at[i])
        pair = parcel[0, i, height:share, :]
        crossed[i, :, rest:panel] = parcel[0, i, 0:height, :]
        crossed[i, low_rows, cut:rest] = turn(pair)
        crossed[i, high_rows, cut:rest] = pair
        send_w[0, row * pieces + i] = three_pass_last(fold[0, 0, 0], local[i]) + three_pass_last(
            fold[0, 0, 1, :, cut:panel], crossed[i, :, cut:panel]
        )
        spread(0, i)
        convert(i)
        return _

    lax.fori_loop(0, pieces, fold_right, 0)
    last = pieces - 1
    mark = last * (blocks // pieces) * width
    settle(target, target_sem.at[0])
    forward_right(0, last)

    @pl.when(core == 1)
    def _():
        forward_right(last, pieces)

    settle(buffer(0).at[pl.ds(0, 2 * last)], near_recv.at[0])
    split(0, send_cat.at[0], [q for q in range(blocks) if q % pieces < last])
    sums_out[0, 0] = begin(other, 0, 0) - summed(send_cat.at[0], 0, slice(0, mark))

    @pl.when(core == 0)
    def _():
        forward_right(last, pieces)

    settle(buffer(0).at[pl.ds(0, 2)], near_recv.at[3])
    split(0, send_cat.at[0], [q for q in range(blocks) if q % pieces == last])
    sums_out[0, 0] -= summed(send_cat.at[0], 0, slice(mark, None))
    sum_copy(0, 0).start()
    convert(pieces)

    def early(c, carry):
        share_out(0, c)

        @pl.when(c < chunks - pieces)
        def _():
            convert(c + pieces)

        return carry

    lax.fori_loop(1, chunks, early, 0)

    settle(parcel.at[1], cross_recv.at[pieces])

    def fold_left(i, _):
        pair, late_pair = parcel[0, i, height:share, :], parcel[1, i, height:share, :]
        crossed[i, :, 0:cut] = parcel[1, i, 0:height, :]
        crossed[i, low_rows, cut:rest] = jnp.where(is_low, late_pair, turn(pair))
        crossed[i, high_rows, cut:rest] = jnp.where(is_low, turn(late_pair), pair)
        send_w[1, row * pieces + i] = three_pass_last(fold[0, 1, 0], local[i]) + three_pass_last(
            fold[0, 1, 1], crossed[i]
        )
        spread(1, i)
        return _

    lax.fori_loop(0, pieces, fold_left, 0)

    def fold_own(i, _):
        for group in range(2):
            begins = (1 - group) * share
            own_w[row * pieces + i, begins : begins + share, :] = three_pass_last(
                fold[1, group, 0], local[i]
            ) + three_pass_last(fold[1, group, 1], crossed[i])
        spread(2, i)
        return _

    lax.fori_loop(0, pieces, fold_own, 0)
    forward(1)
    collect(1, send_cat.at[1])

    def late(c, _):
        share_out(1, c)
        return _

    lax.fori_loop(0, chunks, late, 0)
    forward(2)
    collect(2, own_cat)

    def mine_too(c, _):
        total = summed(own_cat, c)
        here = pl.ds(pl.multiple_of(c * chunk, chunk), chunk)
        out_ref[0:share, here] = begin(y, 1, c) - total[0:share]
        out_ref[share:panel, here] = begin(y, 0, c) - total[share:panel]
        return _

    lax.fori_loop(0, chunks, mine_too, 0)

    def finish(group, first, last):
        begins = (1 - group) * share

        def step(c, carry):
            here = pl.ds(pl.multiple_of(c * chunk, chunk), chunk)
            out_ref[begins : begins + share, here] += sums_in[group, c]
            return carry

        lax.fori_loop(first, last, step, 0)

    settle(sums_in.at[0], sum_recv.at[0])
    finish(0, 0, chunks)
    settle(send_w.at[:, pl.ds(0, 3 * pieces)], gather_send.at[0])
    settle(own_w.at[pl.ds(0, 3 * pieces)], gather_send.at[1])
    settle(packed, cross_send.at[0])
    settle(sums_in.at[1, pl.ds(0, chunks - 1)], sum_recv.at[1])
    finish(1, 0, chunks - 1)
    settle(sums_in.at[1, chunks - 1], sum_recv.at[2])
    finish(1, chunks - 1, chunks)
    settle(sums_out, sum_send.at[0])


def sweep(trailing, lower_trail, lower_cross, panel_inverse, target):
    rows, blocks, _, width = trailing.shape
    pieces, _, height, _ = lower_trail.shape
    panel = lower_cross.shape[0]
    share = panel // 2
    depth = blocks * width
    chunk = min(ROW_CHUNK, rows // 8)
    chunks = rows // chunk
    held = target.transpose(1, 2, 0).reshape(panel, rows)
    f32, bf16 = jnp.float32, jnp.bfloat16
    vmem, dma = pltpu.VMEM, pltpu.SemaphoreType.DMA
    out = pl.pallas_call(
        sweep_kernel,
        in_specs=[pl.BlockSpec(memory_space=pl.ANY)] * 5,
        out_specs=pl.BlockSpec(memory_space=pltpu.VMEM),
        out_shape=vmem((panel, rows), f32),
        scratch_shapes=[
            vmem((2, blocks, chunk, width), f32),
            vmem((rows, depth), bf16),
            vmem((rows, depth), bf16),
            vmem((pieces, height, panel), f32),
            vmem((pieces, height, panel), f32),
            vmem((2, pieces, share, LANES), f32),
            vmem((2, pieces, share, LANES), f32),
            vmem((pieces, height, panel), f32),
            vmem((2, panel, panel), f32),
            vmem((panel, panel), f32),
            vmem((chunks, panel, chunk), f32),
            vmem((3, panel, panel), f32),
            vmem((3, panel, share), f32),
            vmem((2, 2, 2, share, panel), f32),
            vmem((2, blocks, share, width), f32),
            vmem((blocks, panel, width), f32),
            vmem((2, panel, depth), bf16),
            vmem((2 * panel, depth), bf16),
            vmem((2, chunks, share, chunk), f32),
            vmem((2, chunks, share, chunk), f32),
            dma((2,)),
            dma((4,)),
            dma((1,)),
            dma((1,)),
            dma((pieces + 1,)),
            dma((2,)),
            dma((pieces + 2,)),
            dma((4,)),
            dma((1,)),
            dma((3,)),
        ],
        compiler_params=pltpu.CompilerParams(
            collective_id=0, has_side_effects=True, vmem_limit_bytes=58 * 1024 * 1024
        ),
    )(trailing.reshape(rows, blocks, width), lower_trail, lower_cross, panel_inverse, held)
    return out.reshape(2, share, rows).transpose(2, 0, 1)


def fits(trailing, lower_trail, lower_cross):
    rows, blocks, _, width = trailing.shape
    pieces, owners, height, held = lower_trail.shape
    panel = lower_cross.shape[0]
    return (
        lax.axis_size("row") == 4
        and lax.axis_size("col") == 2
        and owners == 2
        and held == panel
        and height == width == LANES
        and blocks == 4 * pieces
        and panel == 2 * (height + height // 2)
        and rows % (8 * LANES) == 0
        and rows // min(ROW_CHUNK, rows // 8) == 2 * pieces
    )


def per_device(trailing, lower_trail, lower_cross, panel_inverse, target):
    if fits(trailing, lower_trail, lower_cross):
        return sweep(trailing, lower_trail, lower_cross, panel_inverse, target)
    cols = lax.axis_size("col")
    me = lax.axis_index("col")
    rows, blocks, _, width = trailing.shape
    depth = lower_trail.shape[0] * width
    panel = lower_cross.shape[0]
    span = 2 * panel
    share = panel // cols
    out_cols = 2 * share
    held = span // cols

    def shift(array, step):
        if step == 0:
            return array
        return lax.ppermute(array, "col", [(i, (i + step) % cols) for i in range(cols)])

    pieces = []
    for step in range(cols):
        block = lax.dynamic_index_in_dim(lower_trail, (me + step) % cols, 1, keepdims=False)
        pieces.append(shift(block, step).reshape(depth, held))

    left, right = panel_inverse[0], panel_inverse[1]
    cross = matmul(matmul(right, lower_cross, exact), left, exact)
    top = jnp.concatenate([left.T, -cross.T], axis=1)
    bottom = jnp.concatenate([jnp.zeros_like(left), right.T], axis=1)
    by_owner = jnp.stack([top, bottom]).reshape(2, cols, share, span)

    def owner_fold(owner):
        return lax.dynamic_index_in_dim(by_owner, owner, 1, keepdims=False).reshape(out_cols, span)

    def gathered(fold, part):
        total = None
        for back, piece in enumerate(pieces):
            source = (me - back) % cols
            weights = lax.dynamic_slice_in_dim(fold[part], source * held, held, 1)
            term = contract_last(piece, weights)
            total = term if total is None else total + term
        return lax.all_gather(total, "row", axis=0, tiled=True)

    held_col = jnp.arange(out_cols)
    place = (held_col // share) * panel + me * share + held_col % share
    pick = (place[:, None] == jnp.arange(span)[None, :]).astype(jnp.float32)

    trail = trailing.reshape(rows, blocks, width)
    own_target = target.transpose(1, 2, 0).reshape(out_cols, rows)
    first = LANES if out_cols > LANES else out_cols
    parts = [slice(0, first)] + ([slice(first, out_cols)] if first < out_cols else [])
    folds = [owner_fold((me + step) % cols) for step in range(cols)]
    factors = {}
    for step in range(1, cols):
        for index, part in enumerate(parts):
            factors[step, index] = gathered(folds[step], part)
    own_factor = gathered(folds[0], slice(0, out_cols))

    chunks = CHUNKS if rows % (CHUNKS * LANES) == 0 else 1
    arrived = [[[] for _ in range(chunks)] for _ in parts]
    for step in range(1, cols):
        weights = contract_last(folds[step], pick, exact)
        for index, part in enumerate(parts):
            for chunk in range(chunks):
                partial = share_of(trail, factors[step, index], weights[part], own_target, chunk, chunks)
                arrived[index][chunk].append(shift(partial, step))
    own = share_of(trail, own_factor, contract_last(folds[0], pick, exact), own_target)
    if cols == 1:
        return own.reshape(2, share, rows).transpose(2, 0, 1)
    others = []
    for pieces_here in arrived:
        sums = [sum(group[1:], group[0]) for group in pieces_here]
        others.append(jnp.concatenate(sums, axis=1))
    result = own + jnp.concatenate(others, axis=0)
    return result.reshape(2, share, rows).transpose(2, 0, 1)


def solution(mesh):
    placed = (
        P(("copy", "row"), None, "col", None),
        P(("copy", "row"), None, None, "col"),
        P(),
        P(),
        P(("copy", "row"), None, "col"),
    )
    return jax.shard_map(
        per_device,
        mesh=mesh,
        in_specs=placed,
        out_specs=P(("copy", "row"), None, "col"),
        check_vma=False,
    )
```
